32 devices in a mesh: visit: 4 (over z), bulk: 8 (over y, x, core).
Axes of the slice: x: 2, y: 2, z: 4, core: 2. Of those that a mesh axis runs over, the one named last changes fastest.
Arguments:
- piece_flux: float32 [4, 8, 8, 128, 128], P('visit', 'bulk'), may hold values from -6 to 6
- piece_ivar: float32 [4, 8, 8, 128, 128], P('visit', 'bulk'), may hold values from 0.5 to 8
- warp_rows: float32 [4, 8, 8, 128, 128], P('visit', 'bulk'), may hold values from 0 to 1, as said below
- warp_cols: float32 [4, 8, 8, 128, 128], P('visit', 'bulk'), may hold values from 0 to 1, as said below
- piece_owner: int32 [4, 8, 8, 1], P('visit', 'bulk'), may hold values from 0 to 7; in each aligned block of 8 rows (0 to 7, 8 to 15, ..., all dimensions but the last counted through in order) at most 2 rows name the same one
- piece_slot: int32 [4, 8, 8], P('visit', 'bulk'), may hold values from 0 to 15
- piece_extent: int32 [4, 8, 8, 2], P('visit', 'bulk'), may hold values from 64 to 128
- basis: float32 [4, 128, 128], replicated, may hold values from -0.046875 to 0.046875
- coeffs: float32 [4, 4], P('visit'), may hold values from -4 to 4
Outputs:
- coadd: float32 [2048, 1024], P('bulk', 'visit')
- weight_map: float32 [2048, 1024], P('bulk', 'visit')
The draws below stay inside these ranges and needn't reach their ends.
Inputs may be any that keep to these rules, and one draw needn't show every extreme that they name: `piece_owner`: among the pieces on one device, no owner is named by more than 2 pieces, a bound that some block reaches. `warp_rows`: entries are nonnegative and each row sums to one. `warp_cols`: entries are nonnegative and each row sums to one.
All inputs are finite; a program needn't handle non-finite values.
Results may differ from the reference program's by a relative error of at most 0.0003.
Values sent between devices are 32-bit elements; how exact they have to be, the bound alone decides.
No kernel may reach another device: no remote copies, remote signals or barrier semaphores. Data moves between devices by JAX's collectives and lax.ppermute only.
A program may use at most 128 MiB of HBM per device.

```python
import math
import jax
import jax.numpy as jnp
import numpy as np
from jax import lax

S = 128
HALO = 64
BR = 2
BC = 8
CAP = 2
BASES = 4
VISITS = 4
OWNERS = 8
PIECES_DEV = 8
COLS = 1024
NROWS = 2048
KS = 128


def dense_warp(key):
    full_shape = (VISITS, OWNERS, PIECES_DEV, S, S)
    key_diag, key_side = jax.random.split(key)
    positions = jnp.arange(S, dtype=jnp.int32)
    on_diag = positions[:, None] == positions[None, :]
    diagonal = jax.random.uniform(key_diag, full_shape, jnp.float32, 1.5, 2.5)
    side_vals = jax.random.uniform(key_side, full_shape, jnp.float32, 0.0, 2.0 / S)
    matrix = jnp.where(on_diag, diagonal, side_vals)
    return matrix / jnp.sum(matrix, axis=-1, keepdims=True)


def draw_warp_rows(key, part):
    return dense_warp(jax.random.fold_in(key, 11))


def draw_warp_cols(key, part):
    return dense_warp(jax.random.fold_in(key, 23))


def set_ends(values, key, least, largest):
    longest = values.shape.index(max(values.shape))
    spots = []
    for shift in (0, 1):
        where = [jax.random.randint(jax.random.fold_in(key, axis), (), 0, length) for axis, length in enumerate(values.shape)]
        where[longest] = (where[longest] + shift) % values.shape[longest]
        spots.append(tuple(where))
    return values.at[spots[0]].set(least).at[spots[1]].set(largest)


def block_scale(key, dims, cuts, smallest, high):
    level = 1.0
    for dim, blocks in cuts:
        draws = jax.random.uniform(jax.random.fold_in(jax.random.fold_in(key, 6), dim), (blocks,), jnp.float32, smallest / len(cuts), high / len(cuts))
        level = level * jnp.repeat(jnp.exp(draws), dims[dim] // blocks).reshape((-1,) + (1,) * (len(dims) - 1 - dim))
    return level


def deal_out(stream_key, own, number, rows, amount, top, limit, slope):
    sequence = jax.random.permutation(stream_key, amount)
    packed, usual = portions_of(amount, rows * top, limit, slope, True), portions_of(amount, rows * top, limit, slope, False)
    places = jnp.arange(amount)

    def named(lengths, rotation):
        used = int((lengths > 0).sum())
        fixed = max(1, used // 4)
        moved = fixed + (places - fixed + rotation * (used - fixed)) % max(1, amount - fixed)
        return jnp.zeros((amount,), jnp.int32).at[sequence[jnp.where(places < fixed, places, moved)]].set(jnp.asarray(lengths, jnp.int32))

    lengths = jnp.where(number % 4 == 0, named(packed, number // 4), named(usual, number - number // 4 - 1))
    mixed = jax.random.permutation(jax.random.fold_in(own, 3), amount)
    source_of, sink = mixed[0:amount // 2 * 2:2], mixed[1:amount // 2 * 2:2]
    margin = jnp.minimum(lengths[source_of] - 1, limit - lengths[sink]) // 2
    margin = jnp.where((source_of == sequence[0]) | (sink == sequence[0]) | (lengths[sink] == 0), 0, jnp.maximum(margin, 0))
    moved = jax.random.randint(jax.random.fold_in(own, 4), (amount // 2,), 0, 1 << 20) % (margin + 1)
    lengths = lengths.at[source_of].add(-moved).at[sink].add(moved)
    members = jnp.searchsorted(jnp.cumsum(lengths), jnp.arange(rows * top), side="right").astype(jnp.int32)
    table = members.reshape(top, rows).T
    table = table[jax.random.permutation(jax.random.fold_in(own, 1), rows)]
    rotation = jax.random.randint(jax.random.fold_in(own, 2), (rows, 1), 0, top)
    return jnp.take_along_axis(table, (jnp.arange(top)[None, :] + rotation) % top, axis=1)


def portions_of(amount, total, reach, skew, full):
    portions = [(1 << 20) // math.isqrt(grade ** skew) + 1 for grade in range(1, amount + 1)]
    largest = reach if full else min(reach, max(-(-total // amount), total * portions[0] // sum(portions)))
    least = 1 if total - largest >= amount - 1 else 0
    counts, surplus = [largest] + [least] * (amount - 1), total - largest - least * (amount - 1)
    while surplus > 0:
        free = [i for i in range(1, amount) if counts[i] < largest] or [i for i in range(1, amount) if counts[i] < reach]
        pool, remaining = sum([portions[i] for i in free]), surplus
        for i in free:
            more = min(reach - counts[i], max(1, remaining * portions[i] // pool), surplus)
            counts[i] = counts[i] + more
            surplus = surplus - more
    return np.array(counts)


def centred(key, shape, deviation, limit, cuts=(), kind=jnp.bfloat16):
    factor_of = block_scale(key, shape, cuts, -0.22, 0.18) if cuts else 1.0
    drawn = jax.random.normal(key, shape, jnp.float32) * deviation * factor_of
    return jnp.minimum(jnp.maximum(drawn, -limit), limit).astype(kind)


def setup_inputs(seed: int = 0) -> dict:
    splits = jax.random.split(jax.random.key(seed), 10)
    piece_flux = centred(splits[0], (VISITS, OWNERS, PIECES_DEV, S, S), 1.0, 6.0, ((0, 4), (1, 8)), jnp.float32)
    piece_ivar = jnp.clip(jnp.exp(math.log(8.0) - 2.7725887 * jax.random.uniform(splits[1], (VISITS, OWNERS, PIECES_DEV, S, S), jnp.float32) ** block_scale(splits[1], (VISITS, OWNERS, PIECES_DEV, S, S), ((0, 4), (1, 8)), -0.2, 0.2)), 0.5, 8.0)
    warp_rows = draw_warp_rows(jax.random.fold_in(splits[9], 71), 0)
    warp_cols = draw_warp_cols(jax.random.fold_in(splits[9], 71), 0)
    piece_owner_keys = jax.random.split(jax.random.fold_in(splits[4], 1), VISITS * OWNERS * PIECES_DEV // PIECES_DEV)
    piece_owner_turns = jax.random.permutation(jax.random.fold_in(splits[4], 3), VISITS * OWNERS * PIECES_DEV // PIECES_DEV)
    piece_owner = jax.vmap(lambda own, number: deal_out(jax.random.fold_in(splits[4], 2), own, number, PIECES_DEV, OWNERS, 1, CAP, 2))(piece_owner_keys, piece_owner_turns).reshape((VISITS, OWNERS, PIECES_DEV, 1))
    piece_slot = set_ends(jax.random.randint(splits[5], (VISITS, OWNERS, PIECES_DEV), 0, BR * BC), jax.random.fold_in(splits[5], 1), 0, (BR * BC) - 1).astype(jnp.int32)
    piece_extent = set_ends(jax.random.randint(splits[6], (VISITS, OWNERS, PIECES_DEV, 2), S // 2, S + 1), jax.random.fold_in(splits[6], 1), S // 2, S).astype(jnp.int32)
    basis = centred(splits[7], (BASES, KS, KS), (KS * KS) ** -0.5, 0.046875, (), jnp.float32)
    coeffs = centred(splits[8], (VISITS, BASES), 1.0, 4.0, ((0, 4),), jnp.float32)
    return dict(piece_flux=piece_flux, piece_ivar=piece_ivar, warp_rows=warp_rows, warp_cols=warp_cols, piece_owner=piece_owner, piece_slot=piece_slot, piece_extent=piece_extent, basis=basis, coeffs=coeffs)


HIGHEST_PREC = lax.Precision.HIGHEST


def warp_pieces(flux_data, ivar_data, row_maps, col_maps, extent):
    positions = jnp.arange(flux_data.shape[-1], dtype=jnp.int32)
    row_ok = positions[None, :, None] < extent[:, 0][:, None, None]
    col_ok = positions[None, None, :] < extent[:, 1][:, None, None]
    valid_mask = jnp.where(row_ok & col_ok, 1.0, 0.0).astype(flux_data.dtype)
    weighted = valid_mask * ivar_data
    planes = jnp.stack([weighted * flux_data, weighted], axis=1)
    inner = jnp.einsum("qcij,qkj->qcik", planes, col_maps, precision=HIGHEST_PREC)
    return jnp.einsum("qij,qcjk->qcik", row_maps, inner, precision=HIGHEST_PREC)


def match_psf(visit_image, kernel):
    row_total = visit_image.shape[0] + 2 * HALO
    col_total = visit_image.shape[1] + 2 * HALO
    padded = jnp.pad(visit_image, ((0, 2 * HALO), (0, 2 * HALO)))
    kernel_pad = jnp.pad(kernel, ((0, row_total - 2 * HALO), (0, col_total - 2 * HALO)))
    kernel_pad = jnp.roll(kernel_pad, (-HALO, -HALO), (0, 1))
    spectrum = jnp.fft.rfft2(padded) * jnp.fft.rfft2(kernel_pad)
    result = jnp.fft.irfft2(spectrum, s=(row_total, col_total))
    return result[:visit_image.shape[0], :visit_image.shape[1]].astype(visit_image.dtype)


def reference(piece_flux, piece_ivar, warp_rows, warp_cols, piece_owner, piece_slot, piece_extent, basis, coeffs):
    pieces = OWNERS * PIECES_DEV
    blocks = BR * BC

    def add_visit(totals, visit_data):
        flux_data, ivar_data, row_maps, col_maps, owner_idx, slot_idx, extent, weights = visit_data
        warped = warp_pieces(flux_data.reshape(pieces, S, S), ivar_data.reshape(pieces, S, S),
                             row_maps.reshape(pieces, S, S), col_maps.reshape(pieces, S, S),
                             extent.reshape(pieces, 2))
        target = owner_idx.reshape(pieces).astype(jnp.int32) * blocks + slot_idx.reshape(pieces).astype(jnp.int32)
        canvas = jnp.zeros((OWNERS * blocks, 2, S, S), warped.dtype).at[target].add(warped)
        canvas = canvas.reshape(OWNERS, BR, BC, 2, S, S).transpose(3, 0, 1, 4, 2, 5).reshape(2, NROWS, COLS)
        flux_sum = canvas[0]
        ivar_sum = canvas[1]
        visit_image = flux_sum / jnp.maximum(ivar_sum, 1.0)
        kernel = jnp.einsum("k,kij->ij", weights, basis, precision=HIGHEST_PREC)
        matched = match_psf(visit_image, kernel)
        return (totals[0] + ivar_sum * matched, totals[1] + ivar_sum), None

    empty = jnp.zeros((NROWS, COLS), piece_flux.dtype)
    sums, unused = lax.scan(add_visit, (empty, empty),
                            (piece_flux, piece_ivar, warp_rows, warp_cols, piece_owner, piece_slot, piece_extent, coeffs))
    numerator, weight_map = sums
    coadd = numerator / jnp.maximum(weight_map, 1.0)
    return coadd, weight_map
```

```python
import functools
import math

import jax
import jax.numpy as jnp
import numpy as np
from jax import lax
from jax.experimental import pallas as pl
from jax.experimental.pallas import tpu as pltpu
from jax.sharding import PartitionSpec as P

HALO = 64
BR = 2
BC = 8
CAP = 2
LANES = 128
META = 8

F32 = jnp.float32
BF16 = jnp.bfloat16
VMEM = pl.BlockSpec(memory_space=pltpu.VMEM)
SMEM = pl.BlockSpec(memory_space=pltpu.SMEM)


def split(value):
    high = value.astype(BF16)
    low = (value - high.astype(F32)).astype(BF16)
    return high, low


def split_table(table):
    table = np.asarray(table, np.float32)
    high = table.astype(jnp.bfloat16)
    low = (table - high.astype(np.float32)).astype(jnp.bfloat16)
    return np.stack([high, low])


def dot(a, b, dims=((1,), (0,))):
    return lax.dot_general(a, b, (dims, ((), ())), preferred_element_type=F32)


def dot3(a, b, dims=((1,), (0,))):
    return dot(a[0], b[0], dims) + dot(a[1], b[0], dims) + dot(a[0], b[1], dims)


def pair(ref):
    return ref[0], ref[1]


@functools.lru_cache
def make_tables(rows_dev, taps):
    length = rows_dev + taps - 1
    freqs = (length + 1) // 2
    k = np.arange(freqs)[:, None]

    def wave(first, second, period):
        return 2.0 * math.pi * ((first * second) % period) / period

    n = np.arange(rows_dev + 2 * HALO)[None, :] - 1
    theta = wave(k, n, length)
    used = n >= 0
    row_fwd = np.concatenate([np.cos(theta) * used, -np.sin(theta) * used], 0)
    theta = wave(k, np.arange(taps)[None, :], length)
    row_ker = np.concatenate([np.cos(theta), -np.sin(theta)], 0)
    period = 2 * taps
    n = np.arange(taps)[:, None]
    f = np.arange(taps)[None, :]
    col_fwd = []
    col_inv = []
    for odd in (0, 1):
        theta = wave(n, 2 * f + odd, period)
        c, s = np.cos(theta), np.sin(theta)
        col_fwd.append(np.block([[c, -s], [s, c]]))
        c, s = c.T, s.T
        sign = -1.0 if odd else 1.0
        col_inv.append(sign * np.block([[c, s], [-s, c]]))
    p = np.arange(rows_dev)[:, None] + taps - 1
    theta = wave(p, k.T, length)
    weight = np.where(k.T == 0, 1.0, 2.0) / (length * period)
    row_inv = np.concatenate([weight * np.cos(theta), -weight * np.sin(theta)], 1)
    return (
        split_table(row_fwd),
        split_table(row_ker),
        np.concatenate([split_table(t) for t in col_fwd]),
        np.concatenate([split_table(t) for t in col_inv]),
        split_table(row_inv),
    )


def warp_body(owner, slot, extent, flux, ivar, rows, cols, outer, inner):
    pieces, side, _ = flux.shape
    half = side // 2
    slots = outer.shape[0]
    for d in range(slots):
        outer[d, side:, :] = jnp.full((META, side), -1.0, F32)
    row_at = lax.broadcasted_iota(jnp.int32, (side, side), 0)
    col_at = lax.broadcasted_iota(jnp.int32, (side, side), 1)
    for q in range(pieces):
        own = owner[q]
        rank = jnp.int32(0)
        for earlier in range(q):
            rank = rank + (owner[earlier] == own).astype(jnp.int32)
        dest = own * CAP + rank
        first = (slot[q] // BC) * half
        valid = (row_at < extent[q, 0]) & (col_at < extent[q, 1])
        weighted = jnp.where(valid, ivar[q], 0.0)
        planes = jnp.concatenate([weighted * flux[q], weighted], 0)
        mid = dot3(split(planes), split(cols[q]), ((1,), (1,)))
        mid = jnp.concatenate([mid[:side], mid[side:]], 1)
        maps = jnp.concatenate([rows[q, pl.ds(first, half), :], rows[q, pl.ds(half - first, half), :]], 0)
        done = dot3(split(maps), split(mid))
        outer[dest, :half, :] = done[:half, :side]
        outer[dest, half:side, :] = done[:half, side:]
        outer[dest, side:, :] = jnp.full((META, side), slot[q].astype(F32), F32)
        inner[dest, :half, :] = done[half:, :side]
        inner[dest, half:, :] = done[half:, side:]


def place(got, slots, acc_f, acc_w):
    half = acc_f.shape[1]
    acc_f[...] = jnp.zeros(acc_f.shape, F32)
    acc_w[...] = jnp.zeros(acc_w.shape, F32)
    for q, at in enumerate(slots):

        @pl.when(at >= 0)
        def _():
            acc_f[at] += got[q, :half, :]
            acc_w[at] += got[q, half : 2 * half, :]


def outer_body(visit, got, top, bottom, ivar_rel, slot_out, acc_f, acc_w):
    count, side, _ = got.shape
    side = side - META
    half = side // 2
    visits, per_tile = ivar_rel.shape[:2]
    slots = []
    for q in range(count):
        at = jnp.max(got[q, side:, :]).astype(jnp.int32)
        slot_out[q] = at
        slots.append(at)
    place(got, slots, acc_f, acc_w)
    me = visit[0]
    for c in range(BC):
        rel = lax.rem(c // per_tile + visits - me, visits)
        w0, w1 = acc_w[c], acc_w[BC + c]
        top[c] = acc_f[c] / jnp.maximum(w0, 1.0)
        bottom[c] = acc_f[BC + c] / jnp.maximum(w1, 1.0)
        ivar_rel[rel, c % per_tile, :half, :] = w0
        ivar_rel[rel, c % per_tile, half:, :] = w1


def inner_body(visit, slot, got, image, ivar_rel, acc_f, acc_w):
    count, side, _ = got.shape
    half = side // 2
    visits, per_tile = ivar_rel.shape[:2]
    place(got, [slot[q] for q in range(count)], acc_f, acc_w)
    me = visit[0]
    for c in range(BC):
        rel = lax.rem(c // per_tile + visits - me, visits)
        w0, w1 = acc_w[c], acc_w[BC + c]
        image[c, :half, :] = acc_f[c] / jnp.maximum(w0, 1.0)
        image[c, half:, :] = acc_f[BC + c] / jnp.maximum(w1, 1.0)
        ivar_rel[rel, c % per_tile, :half, :] = w0
        ivar_rel[rel, c % per_tile, half:, :] = w1


def beside(stacked):
    n = stacked.shape[0] // 2
    return jnp.concatenate([stacked[:n], stacked[n:]], 1)


def spectrum_body(coeffs, basis, row_ker, col_fwd, out):
    kernel = coeffs[0, 0] * basis[0]
    for k in range(1, basis.shape[0]):
        kernel = kernel + coeffs[0, k] * basis[k]
    lines = split(beside(dot3(pair(row_ker), split(kernel))))
    for odd in (0, 1):
        out[odd] = dot3(lines, (col_fwd[2 * odd], col_fwd[2 * odd + 1]))


def conv_body(
    visit, above, top, image, bottom, below, ivar_o, ivar_i, spec, row_fwd, col_fwd, col_inv, row_inv,
    num_o, num_i, lines,
):
    half = top.shape[1]
    taps = top.shape[2]
    visits, per_tile = ivar_o.shape[:2]
    freqs = lines.shape[1] // 2
    table = pair(row_fwd)
    blocks = BC + 1

    def column(c):
        return jnp.concatenate([above[c], top[c], image[c], bottom[c], below[c]], 0)

    gap = jnp.zeros((row_fwd.shape[2], HALO), F32)

    def shifted(u):
        left = column(u - 1)[:, taps - HALO :] if u > 0 else gap
        right = column(u)[:, :HALO] if u < BC else gap
        return jnp.concatenate([left, right], 1)

    for u in range(0, blocks, 2):
        n = min(2, blocks - u)
        ext = jnp.concatenate([shifted(u + i) for i in range(n)], 1)
        got = dot3(table, split(ext))
        for i in range(n):
            lines[u + i] = got[:, i * taps : (i + 1) * taps]

    me = visit[0]
    group = max(2, per_tile)
    for first in range(0, visits * per_tile, group):
        at = []
        for g in range(first, first + group):
            at.append(lax.rem(g // per_tile + me, visits) * per_tile + g % per_tile)
        one = [lines[a] for a in at]
        two = [lines[a + 1] for a in at]
        total = []
        for odd in (0, 1):
            mixed = [beside(a - b if odd else a + b) for a, b in zip(one, two)]
            freq = dot3(split(jnp.concatenate(mixed, 0)), (col_fwd[2 * odd], col_fwd[2 * odd + 1]))
            kr = jnp.concatenate([spec[odd, :, :taps]] * group, 0)
            ki = jnp.concatenate([spec[odd, :, taps:]] * group, 0)
            zr, zi = freq[:, :taps], freq[:, taps:]
            prod = jnp.concatenate([zr * kr - zi * ki, zr * ki + zi * kr], 1)
            total.append(dot3(split(prod), (col_inv[2 * odd], col_inv[2 * odd + 1])))
        wave = total[0] + total[1]
        cols = [
            jnp.concatenate([wave[g * freqs : (g + 1) * freqs, :taps], wave[g * freqs : (g + 1) * freqs, taps:]], 0)
            for g in range(group)
        ]
        out = dot3(pair(row_inv), split(jnp.concatenate(cols, 1)))
        for i in range(group):
            r, c = divmod(first + i, per_tile)
            part = out[:, i * taps : (i + 1) * taps]
            num_o[r, c, :half, :] = part[:half] * ivar_o[r, c, :half, :]
            num_i[r, c] = part[half:-half] * ivar_i[r, c]
            num_o[r, c, half:, :] = part[-half:] * ivar_o[r, c, half:, :]


def final_body(parts_n, parts_d, coadd, weight):
    pass


def ring_sum(outer, inner, axis):
    count = outer.shape[0]
    right = [(i, (i + 1) % count) for i in range(count)]
    left = [((i + 1) % count, i) for i in range(count)]
    far = count // 2
    if count == 1:
        return [outer[0]], [inner[0]]
    to_right = lax.ppermute(outer[far], axis, right)
    to_left = lax.ppermute(inner[far], axis, left)
    sent_r, sent_l = None, None
    for k in range(far - 1, 0, -1):
        ro, ri = outer[k], inner[k]
        lo, li = outer[count - k], inner[count - k]
        if sent_r is None:
            ro = ro + to_right
            li = li + to_left
        else:
            ro, ri = ro + sent_r[0], ri + sent_r[1]
            lo, li = lo + sent_l[0], li + sent_l[1]
        sent_r = lax.ppermute(jnp.stack([ro, ri]), axis, right)
        sent_l = lax.ppermute(jnp.stack([lo, li]), axis, left)
    if sent_r is None:
        return [outer[0], to_right], [inner[0], to_left]
    return [outer[0], sent_r[0], sent_l[0]], [inner[0], sent_r[1], sent_l[1]]


def on_device(piece_flux, piece_ivar, warp_rows, warp_cols, piece_owner, piece_slot, piece_extent, basis, coeffs):
    owners = lax.axis_size("bulk")
    visits = lax.axis_size("visit")
    pieces, side = piece_flux.shape[2:4]
    half = side // 2
    assert half == HALO and BR == 2 and side == LANES
    rows_dev = BR * side
    per_tile = BC // visits
    cap = owners * CAP
    tables = [jnp.asarray(t) for t in make_tables(rows_dev, side)]
    row_fwd, row_ker, col_fwd, col_inv, row_inv = tables
    freqs = row_fwd.shape[1] // 2
    visit = lax.axis_index("visit").astype(jnp.int32).reshape(1)

    def arr(*shape):
        return jax.ShapeDtypeStruct(shape, F32)

    outer, inner = pl.pallas_call(
        warp_body,
        out_shape=(arr(cap, side + META, side), arr(cap, side, side)),
        in_specs=[SMEM] * 3 + [VMEM] * 4,
        out_specs=(VMEM, VMEM),
        name="warp",
    )(
        piece_owner.reshape(pieces),
        piece_slot.reshape(pieces),
        piece_extent.reshape(pieces, 2),
        piece_flux.reshape(pieces, side, side),
        piece_ivar.reshape(pieces, side, side),
        warp_rows.reshape(pieces, side, side),
        warp_cols.reshape(pieces, side, side),
    )
    got_outer = lax.all_to_all(outer, "bulk", split_axis=0, concat_axis=0, tiled=True)
    got_inner = lax.all_to_all(inner, "bulk", split_axis=0, concat_axis=0, tiled=True)
    spec = pl.pallas_call(
        spectrum_body,
        out_shape=arr(2, freqs, 2 * side),
        in_specs=[SMEM] + [VMEM] * 3,
        out_specs=VMEM,
        name="spectrum",
    )(coeffs, basis, row_ker, col_fwd)
    scratch = [pltpu.VMEM((BR * BC, half, side), F32)] * 2
    top, bottom, ivar_o, slots = pl.pallas_call(
        outer_body,
        out_shape=(
            arr(BC, half, side),
            arr(BC, half, side),
            arr(visits, per_tile, side, side),
            jax.ShapeDtypeStruct((cap,), jnp.int32),
        ),
        in_specs=[SMEM, VMEM],
        out_specs=(VMEM, VMEM, VMEM, SMEM),
        scratch_shapes=scratch,
        name="outer",
    )(visit, got_outer)
    ends = owners - 1
    above = lax.ppermute(bottom, "bulk", [(i, i + 1) for i in range(ends)])
    below = lax.ppermute(top, "bulk", [(i + 1, i) for i in range(ends)])
    image, ivar_i = pl.pallas_call(
        inner_body,
        out_shape=(arr(BC, side, side), arr(visits, per_tile, side, side)),
        in_specs=[SMEM, SMEM, VMEM],
        out_specs=(VMEM, VMEM),
        scratch_shapes=scratch,
        name="inner",
    )(visit, slots, got_inner)
    den_o, den_i = ring_sum(ivar_o, ivar_i, "visit")
    num_o, num_i = pl.pallas_call(
        conv_body,
        out_shape=(arr(visits, per_tile, side, side), arr(visits, per_tile, side, side)),
        in_specs=[SMEM] + [VMEM] * 12,
        out_specs=(VMEM, VMEM),
        scratch_shapes=[pltpu.VMEM((BC + 1, 2 * freqs, side), F32)],
        name="conv",
    )(visit, above, top, image, bottom, below, ivar_o, ivar_i, spec, row_fwd, col_fwd, col_inv, row_inv)
    sum_o, sum_i = ring_sum(num_o, num_i, "visit")

    def assemble(outer_parts, inner_parts):
        o = functools.reduce(jnp.add, outer_parts)
        i = functools.reduce(jnp.add, inner_parts)
        tile = jnp.concatenate([o[:, :half], i, o[:, half:]], 1)
        return tile.transpose(1, 0, 2).reshape(rows_dev, per_tile * side)

    weight = assemble(den_o, den_i)
    coadd = assemble(sum_o, sum_i) / jnp.maximum(weight, 1.0)
    return (coadd, weight)


def solution(mesh):
    placed = (
        P("visit", "bulk", None, None, None),
        P("visit", "bulk", None, None, None),
        P("visit", "bulk", None, None, None),
        P("visit", "bulk", None, None, None),
        P("visit", "bulk", None, None),
        P("visit", "bulk", None),
        P("visit", "bulk", None, None),
        P(),
        P("visit", None),
    )
    return jax.shard_map(
        on_device,
        mesh=mesh,
        in_specs=placed,
        out_specs=(P("bulk", "visit"), P("bulk", "visit")),
        check_vma=False,
    )
```

```python
import functools
import math

import jax
import jax.numpy as jnp
import numpy as np
from jax import lax
from jax.experimental import pallas as pl
from jax.experimental.pallas import tpu as pltpu
from jax.sharding import PartitionSpec as P

HALO = 64
BR = 2
BC = 8
CAP = 2
LANES = 128
META = 8


F32 = jnp.float32
BF16 = jnp.bfloat16
VMEM = pl.BlockSpec(memory_space=pltpu.VMEM)
SMEM = pl.BlockSpec(memory_space=pltpu.SMEM)


def split(value):
    high = value.astype(BF16)
    low = (value - high.astype(F32)).astype(BF16)
    return high, low


def split_table(table):
    table = np.asarray(table, np.float32)
    high = table.astype(jnp.bfloat16)
    low = (table - high.astype(np.float32)).astype(jnp.bfloat16)
    return np.stack([high, low])


def dot(a, b, dims=((1,), (0,))):
    return lax.dot_general(a, b, (dims, ((), ())), preferred_element_type=F32)


def dot3(a, b, dims=((1,), (0,))):
    return dot(a[0], b[0], dims) + dot(a[1], b[0], dims) + dot(a[0], b[1], dims)


def pair(ref):
    return ref[0], ref[1]


@functools.lru_cache
def make_tables(rows_dev, taps):
    length = rows_dev + taps - 1
    freqs = (length + 1) // 2
    k = np.arange(freqs)[:, None]

    def wave(first, second, period):
        return 2.0 * math.pi * ((first * second) % period) / period

    n = np.arange(rows_dev + 2 * HALO)[None, :] - 1
    theta = wave(k, n, length)
    used = n >= 0
    row_fwd = np.concatenate([np.cos(theta) * used, -np.sin(theta) * used], 0)
    theta = wave(k, np.arange(taps)[None, :], length)
    row_ker = np.concatenate([np.cos(theta), -np.sin(theta)], 0)
    period = 2 * taps
    n = np.arange(taps)[:, None]
    f = np.arange(taps)[None, :]
    col_fwd = []
    col_inv = []
    for odd in (0, 1):
        theta = wave(n, 2 * f + odd, period)
        c, s = np.cos(theta), np.sin(theta)
        col_fwd.append(np.block([[c, -s], [s, c]]))
        c, s = c.T, s.T
        sign = -1.0 if odd else 1.0
        col_inv.append(sign * np.block([[c, s], [-s, c]]))
    p = np.arange(rows_dev)[:, None] + taps - 1
    theta = wave(p, k.T, length)
    weight = np.where(k.T == 0, 1.0, 2.0) / (length * period)
    row_inv = np.concatenate([weight * np.cos(theta), -weight * np.sin(theta)], 1)
    return (
        split_table(row_fwd),
        split_table(row_ker),
        np.concatenate([split_table(t) for t in col_fwd]),
        np.concatenate([split_table(t) for t in col_inv]),
        split_table(row_inv),
    )


def partner(me, other):
    return jnp.bitwise_xor(me, other)


def warp_body(me, owner, slot, extent, flux, ivar, rows, cols, *rest):
    pieces, side, _ = flux.shape[2:]
    owners = len(rest) - 4
    weight_out, flux_out, weight_send, sems = rest[:owners], rest[owners], rest[owners + 1], rest[owners + 2]
    flux_send = rest[owners + 3]
    for d in range(owners):
        for rank in range(CAP):
            weight_send[d, rank, side:, :] = jnp.full((META, side), -1.0, F32)
    row_at = lax.broadcasted_iota(jnp.int32, (side, side), 0)
    col_at = lax.broadcasted_iota(jnp.int32, (side, side), 1)
    for q in range(pieces):
        own = owner[0, 0, q, 0]
        rank = jnp.int32(0)
        for earlier in range(q):
            rank = rank + (owner[0, 0, earlier, 0] == own).astype(jnp.int32)
        to = partner(me[0], own)
        valid = (row_at < extent[0, 0, q, 0]) & (col_at < extent[0, 0, q, 1])
        weighted = jnp.where(valid, ivar[0, 0, q], 0.0)
        planes = jnp.concatenate([weighted * flux[0, 0, q], weighted], 0)
        mid = dot3(split(planes), split(cols[0, 0, q]), ((1,), (1,)))
        mid = jnp.concatenate([mid[:side], mid[side:]], 1)
        done = dot3(split(rows[0, 0, q]), split(mid))
        flux_send[own * CAP + rank] = done[:, :side]
        weight_send[to, rank, :side, :] = done[:, side:]
        weight_send[to, rank, side:, :] = jnp.full((META, side), slot[0, 0, q].astype(F32), F32)
    copies = [pltpu.make_async_copy(weight_send.at[d], weight_out[d], sems.at[d]) for d in range(owners)]
    copies.append(pltpu.make_async_copy(flux_send, flux_out, sems.at[owners]))
    for copy in copies:
        copy.start()
    for copy in copies:
        copy.wait()


def weight_body(me, order, *rest):
    tiles = order.shape[0]
    owners = len(rest) - tiles - 3
    got, out, canvas, slot_out, acc = rest[:owners], rest[owners : owners + tiles], *rest[owners + tiles :]
    side = acc.shape[1]
    per_tile = BC // tiles
    acc[...] = jnp.zeros(acc.shape, F32)
    for d in range(owners):
        source = partner(me[0], d)
        for rank in range(CAP):
            at = jnp.max(got[d][rank, side:, :]).astype(jnp.int32)
            slot_out[source * CAP + rank] = at

            @pl.when(at >= 0)
            def _():
                acc[at] += got[d][rank, :side, :]

    for c in range(BC):
        for r in range(BR):
            canvas[c, r * side : (r + 1) * side, :] = acc[r * BC + c]
    for k in range(tiles):
        for c in range(per_tile):
            for r in range(BR):
                out[k][c, r * side : (r + 1) * side, :] = acc[r * BC + order[k] * per_tile + c]


def image_body(slot, got, canvas, image, top, bottom, acc):
    count, side, _ = got.shape
    acc[...] = jnp.zeros(acc.shape, F32)
    for q in range(count):
        at = slot[q]

        @pl.when(at >= 0)
        def _():
            acc[at] += got[q]

    for c in range(BC):
        for r in range(BR):
            rows = slice(r * side, (r + 1) * side)
            image[c, rows, :] = acc[r * BC + c] / jnp.maximum(canvas[c, rows, :], 1.0)
        top[c] = image[c, :HALO, :]
        bottom[c] = image[c, -HALO:, :]


def beside(stacked):
    n = stacked.shape[0] // 2
    return jnp.concatenate([stacked[:n], stacked[n:]], 1)


def spectrum_body(coeffs, basis, row_ker, col_fwd, out):
    kernel = coeffs[0, 0] * basis[0]
    for k in range(1, basis.shape[0]):
        kernel = kernel + coeffs[0, k] * basis[k]
    lines = split(beside(dot3(pair(row_ker), split(kernel))))
    for odd in (0, 1):
        out[odd] = dot3(lines, (col_fwd[2 * odd], col_fwd[2 * odd + 1]))


def conv_body(first_tile, order, above, image, below, spec, row_fwd, col_fwd, col_inv, row_inv, *rest):
    count = (len(rest) - 1) // 2
    weight, out, lines = rest[:count], rest[count : 2 * count], rest[-1]
    taps = image.shape[2]
    per_tile = weight[0].shape[0]
    table = pair(row_fwd)

    def column(c):
        return jnp.concatenate([above[c], image[c], below[c]], 0)

    def shifted(u):
        left = column(jnp.maximum(u - 1, 0))[:, taps - HALO :]
        right = column(jnp.minimum(u, BC - 1))[:, :HALO]
        left = jnp.where(u > 0, left, 0.0)
        right = jnp.where(u < BC, right, 0.0)
        return jnp.concatenate([left, right], 1)

    one_tile = lines.shape[0] == per_tile + 1
    base = order[first_tile] * per_tile if one_tile else 0
    for u in range(0, lines.shape[0], 2):
        n = min(2, lines.shape[0] - u)
        ext = jnp.concatenate([shifted(jnp.int32(base + u + i)) for i in range(n)], 1)
        got = dot3(table, split(ext))
        for i in range(n):
            lines[u + i] = got[:, i * taps : (i + 1) * taps]
    for k in range(count):
        start = 0 if one_tile else order[first_tile + k] * per_tile
        one = [lines[start + c] for c in range(per_tile)]
        two = [lines[start + c + 1] for c in range(per_tile)]
        freqs = one[0].shape[0] // 2
        total = []
        for odd in (0, 1):
            mixed = [beside(a - b if odd else a + b) for a, b in zip(one, two)]
            freq = dot3(split(jnp.concatenate(mixed, 0)), (col_fwd[2 * odd], col_fwd[2 * odd + 1]))
            kr = jnp.concatenate([spec[odd, :, :taps]] * per_tile, 0)
            ki = jnp.concatenate([spec[odd, :, taps:]] * per_tile, 0)
            zr, zi = freq[:, :taps], freq[:, taps:]
            prod = jnp.concatenate([zr * kr - zi * ki, zr * ki + zi * kr], 1)
            total.append(dot3(split(prod), (col_inv[2 * odd], col_inv[2 * odd + 1])))
        wave = total[0] + total[1]
        parts = [wave[c * freqs : (c + 1) * freqs] for c in range(per_tile)]
        cols = [jnp.concatenate([p[:, :taps], p[:, taps:]], 0) for p in parts]
        done = dot3(pair(row_inv), split(jnp.concatenate(cols, 1)))
        for c in range(per_tile):
            out[k][c] = done[:, c * taps : (c + 1) * taps] * weight[k][c]


def total_body(*refs):
    parts, out = refs[:-1], refs[-1]
    side = parts[0].shape[2]
    for c in range(parts[0].shape[0]):
        out[:, c * side : (c + 1) * side] = functools.reduce(jnp.add, [p[c] for p in parts])


def ratio_body(*refs):
    parts, weight, out = refs[:-2], refs[-2], refs[-1]
    side = parts[0].shape[2]
    for c in range(parts[0].shape[0]):
        cols = slice(c * side, (c + 1) * side)
        out[:, cols] = functools.reduce(jnp.add, [p[c] for p in parts]) / jnp.maximum(weight[:, cols], 1.0)


LINE = ((3, 2, 1, 0), (3, 0, 2, 1), (0, 3, 1, 2), (0, 1, 2, 3))


def send_order(count):
    if count == 4:
        return np.array(LINE, np.int32)
    return np.array([list(range(count))] * count, np.int32)


class VisitSum:
    def __init__(self, count):
        self.count = count
        self.sent = []
        self.tiles = []

    def push(self, *tiles):
        for tile in tiles:
            k = len(self.tiles)
            self.tiles.append(tile)
            if self.count != 4:
                continue
            if k == 0:
                self.sent.append(lax.ppermute(tile, "visit", [(0, 1), (3, 2)]))
            elif k == 1:
                self.sent.append(lax.ppermute(tile, "visit", [(0, 2), (1, 0), (2, 3), (3, 1)]))
            elif k == 2:
                self.sent.append(lax.ppermute(tile, "visit", [(0, 1), (1, 2)]))
                self.sent.append(lax.ppermute(tile, "visit", [(2, 1), (3, 2)]))

    def parts(self):
        if self.count != 4:
            return [lax.psum_scatter(jnp.stack(self.tiles), "visit", scatter_dimension=0, tiled=False)]
        joined = lax.ppermute(self.tiles[0] + self.sent[0], "visit", [(1, 3), (2, 0)])
        return [self.tiles[3], *self.sent[1:], joined]


def on_device(piece_flux, piece_ivar, warp_rows, warp_cols, piece_owner, piece_slot, piece_extent, basis, coeffs):
    owners = lax.axis_size("bulk")
    visits = lax.axis_size("visit")
    pieces, side = piece_flux.shape[2:4]
    assert side == LANES and side == 2 * HALO and owners & (owners - 1) == 0
    rows_dev = BR * side
    per_tile = BC // visits
    cap = owners * CAP
    row_fwd, row_ker, col_fwd, col_inv, row_inv = [jnp.asarray(t) for t in make_tables(rows_dev, side)]
    freqs = row_fwd.shape[1] // 2
    me = lax.axis_index("bulk").astype(jnp.int32).reshape(1)
    order = jnp.asarray(send_order(visits))[lax.axis_index("visit")]

    def arr(*shape):
        return jax.ShapeDtypeStruct(shape, F32)

    hbm = pl.BlockSpec(memory_space=pl.ANY)
    *weights, flux = pl.pallas_call(
        warp_body,
        out_shape=[arr(CAP, side + META, side)] * owners + [arr(cap, side, side)],
        in_specs=[SMEM] * 4 + [VMEM] * 4,
        out_specs=[hbm] * (owners + 1),
        scratch_shapes=[
            pltpu.VMEM((owners, CAP, side + META, side), F32),
            pltpu.SemaphoreType.DMA((owners + 1,)),
            pltpu.VMEM((cap, side, side), F32),
        ],
        name="warp",
    )(me, piece_owner, piece_slot, piece_extent, piece_flux, piece_ivar, warp_rows, warp_cols)
    got = [weights[0]]
    for d in range(1, owners):
        got.append(lax.ppermute(weights[d], "bulk", [(i, i ^ d) for i in range(owners)]))
    got_flux = lax.all_to_all(flux, "bulk", split_axis=0, concat_axis=0, tiled=True)
    spec = pl.pallas_call(
        spectrum_body,
        out_shape=arr(2, freqs, 2 * side),
        in_specs=[SMEM] + [VMEM] * 3,
        out_specs=VMEM,
        name="spectrum",
    )(coeffs, basis, row_ker, col_fwd)
    tile = arr(per_tile, rows_dev, side)
    *ivar, canvas, slots = pl.pallas_call(
        weight_body,
        out_shape=[tile] * visits + [arr(BC, rows_dev, side), jax.ShapeDtypeStruct((cap,), jnp.int32)],
        in_specs=[SMEM] * 2 + [VMEM] * owners,
        out_specs=[VMEM] * (visits + 1) + [SMEM],
        scratch_shapes=[pltpu.VMEM((BR * BC, side, side), F32)],
        name="weights",
    )(me, order, *got)
    weight_sum = VisitSum(visits)
    weight_sum.push(*ivar)
    weight_map = pl.pallas_call(
        total_body, out_shape=arr(rows_dev, per_tile * side), name="weight_map"
    )(*weight_sum.parts())
    image, top, bottom = pl.pallas_call(
        image_body,
        out_shape=(arr(BC, rows_dev, side), arr(BC, HALO, side), arr(BC, HALO, side)),
        in_specs=[SMEM, VMEM, VMEM],
        out_specs=[VMEM] * 3,
        scratch_shapes=[pltpu.VMEM((BR * BC, side, side), F32)],
        name="image",
    )(slots, got_flux, canvas)
    ends = owners - 1
    above = lax.ppermute(bottom, "bulk", [(i, i + 1) for i in range(ends)])
    below = lax.ppermute(top, "bulk", [(i + 1, i) for i in range(ends)])

    def convolve(first, count, blocks, name):
        return pl.pallas_call(
            functools.partial(conv_body, first),
            out_shape=[tile] * count,
            in_specs=[SMEM] + [VMEM] * (8 + count),
            out_specs=[VMEM] * count,
            scratch_shapes=[pltpu.VMEM((blocks, 2 * freqs, side), F32)],
            name=name,
        )(order, above, image, below, spec, row_fwd, col_fwd, col_inv, row_inv, *ivar[first : first + count])

    image_sum = VisitSum(visits)
    image_sum.push(*convolve(0, 1, per_tile + 1, "conv_first"))
    image_sum.push(*convolve(1, visits - 1, BC + 1, "conv_rest"))
    coadd = pl.pallas_call(
        ratio_body, out_shape=arr(rows_dev, per_tile * side), name="coadd"
    )(*image_sum.parts(), weight_map)
    return (coadd, weight_map)


def solution(mesh):
    placed = (
        P("visit", "bulk", None, None, None),
        P("visit", "bulk", None, None, None),
        P("visit", "bulk", None, None, None),
        P("visit", "bulk", None, None, None),
        P("visit", "bulk", None, None),
        P("visit", "bulk", None),
        P("visit", "bulk", None, None),
        P(),
        P("visit", None),
    )
    return jax.shard_map(
        on_device,
        mesh=mesh,
        in_specs=placed,
        out_specs=(P("bulk", "visit"), P("bulk", "visit")),
        check_vma=False,
    )
```

```python
import functools
import math

import jax
import jax.numpy as jnp
import numpy as np
from jax import lax
from jax.experimental import pallas as pl
from jax.experimental.pallas import tpu as pltpu
from jax.sharding import PartitionSpec as P

HALO = 64
BR = 2
BC = 8
CAP = 2
LANES = 128
META = 8


F32 = jnp.float32
BF16 = jnp.bfloat16
VMEM = pl.BlockSpec(memory_space=pltpu.VMEM)
SMEM = pl.BlockSpec(memory_space=pltpu.SMEM)


def split(value):
    high = value.astype(BF16)
    low = (value - high.astype(F32)).astype(BF16)
    return high, low


def data(value, axis):
    high, low = split(value)
    return jnp.concatenate([high, low, high], axis)


def weights(value, axis):
    high, low = split(value)
    return jnp.concatenate([high, high, low], axis)


def table(value, axis):
    value = np.asarray(value, np.float32)
    high = value.astype(jnp.bfloat16)
    low = (value - high.astype(np.float32)).astype(jnp.bfloat16)
    return np.concatenate([high, high, low], axis)


def dot(a, b, dims=((1,), (0,))):
    return lax.dot_general(a, b, (dims, ((), ())), preferred_element_type=F32)


@functools.lru_cache
def make_tables(rows_dev, taps):
    length = rows_dev + taps - 1
    freqs = (length + 1) // 2
    k = np.arange(freqs)[:, None]

    def wave(first, second, period):
        return 2.0 * math.pi * ((first * second) % period) / period

    n = np.arange(rows_dev + 2 * HALO)[None, :] - 1
    theta = wave(k, n, length)
    used = n >= 0
    row_fwd = np.concatenate([np.cos(theta) * used, -np.sin(theta) * used], 0)
    theta = wave(k, np.arange(taps)[None, :], length)
    row_ker = np.concatenate([np.cos(theta), -np.sin(theta)], 0)
    period = 2 * taps
    n = np.arange(taps)[:, None]
    f = np.arange(taps)[None, :]
    col_fwd = []
    col_inv = []
    for odd in (0, 1):
        theta = wave(n, 2 * f + odd, period)
        c, s = np.cos(theta), np.sin(theta)
        col_fwd.append(np.block([[c, -s], [s, c]]))
        c, s = c.T, s.T
        sign = -1.0 if odd else 1.0
        col_inv.append(sign * np.block([[c, s], [-s, c]]))
    p = np.arange(rows_dev)[:, None] + taps - 1
    theta = wave(p, k.T, length)
    weight = np.where(k.T == 0, 1.0, 2.0) / (length * period)
    row_inv = np.concatenate([weight * np.cos(theta), -weight * np.sin(theta)], 1)
    return (
        table(row_fwd, 1),
        table(row_ker, 1),
        np.stack([table(t, 0) for t in col_fwd]),
        np.stack([table(t, 0) for t in col_inv]),
        table(row_inv, 1),
    )


def partner(me, other):
    return jnp.bitwise_xor(me, other)


OWNER, SLOT, ROWS, COLS, ME, ORDER = range(6)


def places(info, pieces):
    for q in range(pieces):
        own = info[OWNER, q]
        rank = jnp.int32(0)
        for earlier in range(q):
            rank = rank + (info[OWNER, earlier] == own).astype(jnp.int32)
        yield q, partner(info[ME, 0], own), own, rank, info[SLOT, q]


def masked(info, ivar, q):
    shape = ivar.shape[3:]
    row_at = lax.broadcasted_iota(jnp.int32, shape, 0)
    col_at = lax.broadcasted_iota(jnp.int32, shape, 1)
    valid = (row_at < info[ROWS, q]) & (col_at < info[COLS, q])
    return jnp.where(valid, ivar[0, 0, q], 0.0)


def warp(plane, rows, cols):
    mid = dot(data(plane, 1), weights(cols, 1), ((1,), (1,)))
    return dot(weights(rows, 1), data(mid, 0))


def run(copies):
    for copy in copies:
        copy.start()
    for copy in copies:
        copy.wait()


def warp_weight_body(info, ivar, rows, cols, *rest):
    pieces, side, _ = ivar.shape[2:]
    *outs, send, sems = rest
    for d in range(len(outs)):
        for rank in range(CAP):
            send[d, rank, side:, :] = jnp.full((META, side), -1.0, F32)
    for q, to, _, rank, at in places(info, pieces):
        send[to, rank, :side, :] = warp(masked(info, ivar, q), rows[0, 0, q], cols[0, 0, q])
        send[to, rank, side:, :] = jnp.full((META, side), at.astype(F32), F32)
    run([pltpu.make_async_copy(send.at[d], out, sems.at[d]) for d, out in enumerate(outs)])


def warp_flux_body(info, flux, ivar, rows, cols, *rest):
    pieces, side, _ = ivar.shape[2:]
    half = side // 2
    *outs, inner, send, send_inner, sems = rest
    for q, to, own, rank, at in places(info, pieces):
        first = (at // BC) * half
        maps = jnp.concatenate([rows[0, 0, q, pl.ds(first, half), :], rows[0, 0, q, pl.ds(half - first, half), :]], 0)
        done = warp(masked(info, ivar, q) * flux[0, 0, q], maps, cols[0, 0, q])
        send[to, rank] = done[:half]
        send_inner[own * CAP + rank] = done[half:]
    copies = [pltpu.make_async_copy(send.at[d], out, sems.at[d]) for d, out in enumerate(outs)]
    run(copies + [pltpu.make_async_copy(send_inner, inner, sems.at[len(outs)])])


def weight_body(info, *rest):
    *rest, slot_out, acc = rest
    count = slot_out.shape[0] // CAP
    got, out = rest[:count], rest[count:]
    side = acc.shape[1]
    spare = acc.shape[0] - 1
    per_tile = out[0].shape[0]
    slots = []
    for d in range(count):
        for rank in range(CAP):
            at = jnp.max(got[d][rank, side:, :]).astype(jnp.int32)
            slots.append(jnp.where(at < 0, spare, at))
    acc[...] = jnp.zeros(acc.shape, F32)
    for n, at in enumerate(slots):
        d, rank = divmod(n, CAP)
        slot_out[partner(info[ME, 0], d) * CAP + rank] = at
        acc[at] += got[d][rank, :side, :]
    for k in range(len(out)):
        for c in range(per_tile):
            for r in range(BR):
                out[k][c, r * side : (r + 1) * side, :] = acc[r * BC + info[ORDER, k] * per_tile + c]


def outer_body(info, slot, *rest):
    *rest, top, bottom, acc = rest
    count = slot.shape[0] // CAP
    got, tiles = rest[:count], rest[count:]
    half = acc.shape[1]
    per_tile = tiles[0].shape[0]
    acc[...] = jnp.zeros(acc.shape, F32)
    for d in range(count):
        for rank in range(CAP):
            acc[slot[partner(info[ME, 0], d) * CAP + rank]] += got[d][rank]
    for k, tile in enumerate(tiles):
        for c in range(per_tile):
            to = info[ORDER, k] * per_tile + c
            top[to] = acc[to] / jnp.maximum(tile[c, :half, :], 1.0)
            bottom[to] = acc[BC + to] / jnp.maximum(tile[c, -half:, :], 1.0)


def inner_body(info, slot, got, *rest):
    *tiles, image, acc = rest
    half = acc.shape[1]
    per_tile = tiles[0].shape[0]
    acc[...] = jnp.zeros(acc.shape, F32)
    for n in range(slot.shape[0]):
        acc[slot[n]] += got[n]
    for k, tile in enumerate(tiles):
        for c in range(per_tile):
            to = info[ORDER, k] * per_tile + c
            image[to, :half, :] = acc[to] / jnp.maximum(tile[c, half : 2 * half, :], 1.0)
            image[to, half:, :] = acc[BC + to] / jnp.maximum(tile[c, 2 * half : 3 * half, :], 1.0)


def beside(stacked):
    n = stacked.shape[0] // 2
    return jnp.concatenate([stacked[:n], stacked[n:]], 1)


def spectrum_body(coeffs, basis, row_ker, col_fwd, out):
    kernel = coeffs[0, 0] * basis[0]
    for k in range(1, basis.shape[0]):
        kernel = kernel + coeffs[0, k] * basis[k]
    lines = data(beside(dot(row_ker[...], data(kernel, 0))), 1)
    for odd in (0, 1):
        out[odd] = dot(lines, col_fwd[odd])


def conv_body(first, info, above, top, image, bottom, below, spec, row_fwd, col_fwd, col_inv, row_inv, *rest):
    *rest, lines = rest
    count = len(rest) // 2
    weight, out = rest[:count], rest[count:]
    taps = image.shape[2]
    per_tile = weight[0].shape[0]

    def column(c):
        return jnp.concatenate([above[c], top[c], image[c], bottom[c], below[c]], 0)

    def shifted(u):
        if isinstance(u, int):
            gap = jnp.zeros((above.shape[1] * 6, HALO), F32)
            left = column(u - 1)[:, taps - HALO :] if u > 0 else gap
            right = column(u)[:, :HALO] if u < BC else gap
            return jnp.concatenate([left, right], 1)
        left = column(jnp.maximum(u - 1, 0))[:, taps - HALO :]
        right = column(jnp.minimum(u, BC - 1))[:, :HALO]
        left = jnp.where(u > 0, left, 0.0)
        right = jnp.where(u < BC, right, 0.0)
        return jnp.concatenate([left, right], 1)

    one_tile = lines.shape[0] == per_tile + 1
    base = info[ORDER, first] * per_tile if one_tile else 0
    for u in range(0, lines.shape[0], 2):
        n = min(2, lines.shape[0] - u)
        ext = jnp.concatenate([shifted(base + u + i) for i in range(n)], 1)
        got = dot(row_fwd[...], data(ext, 0))
        for i in range(n):
            lines[u + i] = got[:, i * taps : (i + 1) * taps]
    for k in range(count):
        start = 0 if one_tile else info[ORDER, first + k] * per_tile
        one = [lines[start + c] for c in range(per_tile)]
        two = [lines[start + c + 1] for c in range(per_tile)]
        freqs = one[0].shape[0] // 2
        total = []
        for odd in (0, 1):
            mixed = [beside(a - b if odd else a + b) for a, b in zip(one, two)]
            freq = dot(data(jnp.concatenate(mixed, 0), 1), col_fwd[odd])
            kr = jnp.concatenate([spec[odd, :, :taps]] * per_tile, 0)
            ki = jnp.concatenate([spec[odd, :, taps:]] * per_tile, 0)
            zr, zi = freq[:, :taps], freq[:, taps:]
            prod = jnp.concatenate([zr * kr - zi * ki, zr * ki + zi * kr], 1)
            total.append(dot(data(prod, 1), col_inv[odd]))
        wave = total[0] + total[1]
        parts = [wave[c * freqs : (c + 1) * freqs] for c in range(per_tile)]
        cols = [jnp.concatenate([p[:, :taps], p[:, taps:]], 0) for p in parts]
        done = dot(row_inv[...], data(jnp.concatenate(cols, 1), 0))
        for c in range(per_tile):
            out[k][c] = done[:, c * taps : (c + 1) * taps] * weight[k][c]


def total_body(*refs):
    parts, out = refs[:-1], refs[-1]
    side = parts[0].shape[2]
    for c in range(parts[0].shape[0]):
        out[:, c * side : (c + 1) * side] = functools.reduce(jnp.add, [p[c] for p in parts])


def ratio_body(*refs):
    parts, weight, out = refs[:-2], refs[-2], refs[-1]
    side = parts[0].shape[2]
    for c in range(parts[0].shape[0]):
        cols = slice(c * side, (c + 1) * side)
        out[:, cols] = functools.reduce(jnp.add, [p[c] for p in parts]) / jnp.maximum(weight[:, cols], 1.0)


LINE = ((3, 2, 1, 0), (3, 0, 2, 1), (0, 3, 1, 2), (0, 1, 2, 3))


def send_order(count):
    if count == 4:
        return np.array(LINE, np.int32)
    return np.array([list(range(count))] * count, np.int32)


class VisitSum:
    def __init__(self, count):
        self.count = count
        self.sent = []
        self.tiles = []

    def push(self, *tiles):
        for tile in tiles:
            k = len(self.tiles)
            self.tiles.append(tile)
            if self.count != 4:
                continue
            if k == 0:
                self.sent.append(lax.ppermute(tile, "visit", [(0, 1), (3, 2)]))
            elif k == 1:
                self.sent.append(lax.ppermute(tile, "visit", [(0, 2), (1, 0), (2, 3), (3, 1)]))
            elif k == 2:
                self.sent.append(lax.ppermute(tile, "visit", [(0, 1), (1, 2)]))
                self.sent.append(lax.ppermute(tile, "visit", [(2, 1), (3, 2)]))

    def parts(self):
        if self.count != 4:
            return [lax.psum_scatter(jnp.stack(self.tiles), "visit", scatter_dimension=0, tiled=False)]
        joined = lax.ppermute(self.tiles[0] + self.sent[0], "visit", [(1, 3), (2, 0)])
        return [self.tiles[3], *self.sent[1:], joined]


def on_device(piece_flux, piece_ivar, warp_rows, warp_cols, piece_owner, piece_slot, piece_extent, basis, coeffs):
    owners = lax.axis_size("bulk")
    visits = lax.axis_size("visit")
    pieces, side = piece_flux.shape[2:4]
    assert side == LANES and side == 2 * HALO and owners & (owners - 1) == 0
    half = side // 2
    rows_dev = BR * side
    per_tile = BC // visits
    cap = owners * CAP
    row_fwd, row_ker, col_fwd, col_inv, row_inv = [jnp.asarray(t) for t in make_tables(rows_dev, side)]
    freqs = row_fwd.shape[0] // 2
    width = max(pieces, visits)

    def line(values):
        return jnp.pad(values, (0, width - values.shape[0]))

    me = lax.axis_index("bulk").astype(jnp.int32)
    order = jnp.asarray(send_order(visits))[lax.axis_index("visit")]
    info = jnp.stack(
        [
            line(piece_owner[0, 0, :, 0]),
            line(piece_slot[0, 0]),
            line(piece_extent[0, 0, :, 0]),
            line(piece_extent[0, 0, :, 1]),
            jnp.full((width,), me),
            line(order),
        ]
    )

    def arr(*shape):
        return jax.ShapeDtypeStruct(shape, F32)

    hbm = pl.BlockSpec(memory_space=pl.ANY)

    def exchange(sent):
        got = [sent[0]]
        for d in range(1, owners):
            got.append(lax.ppermute(sent[d], "bulk", [(i, i ^ d) for i in range(owners)]))
        return got

    sent_weight = pl.pallas_call(
        warp_weight_body,
        out_shape=[arr(CAP, side + META, side)] * owners,
        in_specs=[SMEM] + [VMEM] * 3,
        out_specs=[hbm] * owners,
        scratch_shapes=[pltpu.VMEM((owners, CAP, side + META, side), F32), pltpu.SemaphoreType.DMA((owners,))],
        name="warp_weight",
    )(info, piece_ivar, warp_rows, warp_cols)
    got_weight = exchange(sent_weight)
    *sent_outer, sent_inner = pl.pallas_call(
        warp_flux_body,
        out_shape=[arr(CAP, half, side)] * owners + [arr(cap, half, side)],
        in_specs=[SMEM] + [VMEM] * 4,
        out_specs=[hbm] * (owners + 1),
        scratch_shapes=[
            pltpu.VMEM((owners, CAP, half, side), F32),
            pltpu.VMEM((cap, half, side), F32),
            pltpu.SemaphoreType.DMA((owners + 1,)),
        ],
        name="warp_flux",
    )(info, piece_flux, piece_ivar, warp_rows, warp_cols)
    got_outer = exchange(sent_outer)
    got_inner = lax.all_to_all(sent_inner, "bulk", split_axis=0, concat_axis=0, tiled=True)
    spec = pl.pallas_call(
        spectrum_body,
        out_shape=arr(2, freqs, 2 * side),
        in_specs=[SMEM] + [VMEM] * 3,
        out_specs=VMEM,
        name="spectrum",
    )(coeffs, basis, row_ker, col_fwd)
    tile = arr(per_tile, rows_dev, side)
    *ivar, slots = pl.pallas_call(
        weight_body,
        out_shape=[tile] * visits + [jax.ShapeDtypeStruct((cap,), jnp.int32)],
        in_specs=[SMEM] + [VMEM] * owners,
        out_specs=[VMEM] * visits + [SMEM],
        scratch_shapes=[pltpu.VMEM((BR * BC + 1, side, side), F32)],
        name="weights",
    )(info, *got_weight)
    weight_sum = VisitSum(visits)
    weight_sum.push(*ivar)
    scratch = [pltpu.VMEM((BR * BC + 1, half, side), F32)]
    top, bottom = pl.pallas_call(
        outer_body,
        out_shape=[arr(BC, half, side)] * 2,
        in_specs=[SMEM] * 2 + [VMEM] * (owners + visits),
        out_specs=[VMEM] * 2,
        scratch_shapes=scratch,
        name="outer",
    )(info, slots, *got_outer, *ivar)
    ends = owners - 1
    above = lax.ppermute(bottom, "bulk", [(i, i + 1) for i in range(ends)])
    below = lax.ppermute(top, "bulk", [(i + 1, i) for i in range(ends)])
    image = pl.pallas_call(
        inner_body,
        out_shape=arr(BC, side, side),
        in_specs=[SMEM] * 2 + [VMEM] * (1 + visits),
        out_specs=VMEM,
        scratch_shapes=scratch,
        name="inner",
    )(info, slots, got_inner, *ivar)
    weight_map = pl.pallas_call(
        total_body, out_shape=arr(rows_dev, per_tile * side), name="weight_map"
    )(*weight_sum.parts())

    def convolve(first, count, blocks, name):
        return pl.pallas_call(
            functools.partial(conv_body, first),
            out_shape=[tile] * count,
            in_specs=[SMEM] + [VMEM] * (10 + count),
            out_specs=[VMEM] * count,
            scratch_shapes=[pltpu.VMEM((blocks, 2 * freqs, side), F32)],
            name=name,
        )(
            info, above, top, image, bottom, below, spec, row_fwd, col_fwd, col_inv, row_inv,
            *ivar[first : first + count],
        )

    image_sum = VisitSum(visits)
    image_sum.push(*convolve(0, 1, per_tile + 1, "conv_first"))
    image_sum.push(*convolve(1, visits - 1, BC + 1, "conv_rest"))
    coadd = pl.pallas_call(
        ratio_body, out_shape=arr(rows_dev, per_tile * side), name="coadd"
    )(*image_sum.parts(), weight_map)
    return (coadd, weight_map)


def solution(mesh):
    placed = (
        P("visit", "bulk", None, None, None),
        P("visit", "bulk", None, None, None),
        P("visit", "bulk", None, None, None),
        P("visit", "bulk", None, None, None),
        P("visit", "bulk", None, None),
        P("visit", "bulk", None),
        P("visit", "bulk", None, None),
        P(),
        P("visit", None),
    )
    return jax.shard_map(
        on_device,
        mesh=mesh,
        in_specs=placed,
        out_specs=(P("bulk", "visit"), P("bulk", "visit")),
        check_vma=False,
    )
```

```python
import functools
import math

import jax
import jax.numpy as jnp
import numpy as np
from jax import lax
from jax.experimental import pallas as pl
from jax.experimental.pallas import tpu as pltpu
from jax.sharding import PartitionSpec as P


HALO = 64
BR = 2
BC = 8
CAP = 2
LANES = 128
META = 8


F32 = jnp.float32
BF16 = jnp.bfloat16
VMEM = pl.BlockSpec(memory_space=pltpu.VMEM)
SMEM = pl.BlockSpec(memory_space=pltpu.SMEM)


def split(value):
    high = value.astype(BF16)
    low = (value - high.astype(F32)).astype(BF16)
    return high, low


def data(value, axis):
    high, low = split(value)
    return jnp.concatenate([high, low, high], axis)


def weights(value, axis):
    high, low = split(value)
    return jnp.concatenate([high, high, low], axis)


def table(value, axis):
    value = np.asarray(value, np.float32)
    high = value.astype(jnp.bfloat16)
    low = (value - high.astype(np.float32)).astype(jnp.bfloat16)
    return np.concatenate([high, high, low], axis)


def dot(a, b, dims=((1,), (0,))):
    return lax.dot_general(a, b, (dims, ((), ())), preferred_element_type=F32)


@functools.lru_cache
def make_tables(rows_dev, taps):
    length = rows_dev + taps - 1
    freqs = (length + 1) // 2
    k = np.arange(freqs)[:, None]

    def wave(first, second, period):
        return 2.0 * math.pi * ((first * second) % period) / period

    n = np.arange(rows_dev + 2 * HALO)[None, :] - 1
    theta = wave(k, n, length)
    used = n >= 0
    row_fwd = np.concatenate([np.cos(theta) * used, -np.sin(theta) * used], 0)
    theta = wave(k, np.arange(taps)[None, :], length)
    row_ker = np.concatenate([np.cos(theta), -np.sin(theta)], 0)
    period = 2 * taps
    n = np.arange(taps)[:, None]
    f = np.arange(taps)[None, :]
    col_fwd = []
    col_inv = []
    for odd in (0, 1):
        theta = wave(n, 2 * f + odd, period)
        c, s = np.cos(theta), np.sin(theta)
        col_fwd.append(np.block([[c, -s], [s, c]]))
        c, s = c.T, s.T
        sign = -1.0 if odd else 1.0
        col_inv.append(sign * np.block([[c, s], [-s, c]]))
    p = np.arange(rows_dev)[:, None] + taps - 1
    theta = wave(p, k.T, length)
    weight = np.where(k.T == 0, 1.0, 2.0) / (length * period)
    row_inv = np.concatenate([weight * np.cos(theta), -weight * np.sin(theta)], 1)
    return (
        table(row_fwd, 1),
        table(row_ker, 1),
        np.stack([table(t, 0) for t in col_fwd]),
        np.stack([table(t, 0) for t in col_inv]),
        table(row_inv, 1),
    )


def partner(me, other):
    return jnp.bitwise_xor(me, other)


OWNER, SLOT, ROWS, COLS, ME, ORDER = range(6)


def places(info, pieces):
    for q in range(pieces):
        own = info[OWNER, q]
        rank = jnp.int32(0)
        for earlier in range(q):
            rank = rank + (info[OWNER, earlier] == own).astype(jnp.int32)
        yield q, partner(info[ME, 0], own), own, rank, info[SLOT, q]


def masked(info, ivar, q):
    shape = ivar.shape[3:]
    row_at = lax.broadcasted_iota(jnp.int32, shape, 0)
    col_at = lax.broadcasted_iota(jnp.int32, shape, 1)
    valid = (row_at < info[ROWS, q]) & (col_at < info[COLS, q])
    return jnp.where(valid, ivar[0, 0, q], 0.0)


def warp(plane, rows, cols):
    mid = dot(data(plane, 1), weights(cols, 1), ((1,), (1,)))
    return dot(weights(rows, 1), data(mid, 0))


def run(copies):
    for copy in copies:
        copy.start()
    for copy in copies:
        copy.wait()


def warp_weight_body(info, ivar, rows, cols, *rest):
    pieces, side, _ = ivar.shape[2:]
    *outs, send, sems = rest
    for d in range(len(outs)):
        for rank in range(CAP):
            send[d, rank, side:, :] = jnp.full((META, side), -1.0, F32)
    for q, to, _, rank, at in places(info, pieces):
        send[to, rank, :side, :] = warp(masked(info, ivar, q), rows[0, 0, q], cols[0, 0, q])
        send[to, rank, side:, :] = jnp.full((META, side), at.astype(F32), F32)
    run([pltpu.make_async_copy(send.at[d], out, sems.at[d]) for d, out in enumerate(outs)])


def warp_flux_body(info, flux, ivar, rows, cols, *rest):
    pieces, side, _ = ivar.shape[2:]
    half = side // 2
    *outs, inner, send, send_inner, sems = rest
    for q, to, own, rank, at in places(info, pieces):
        first = (at // BC) * half
        maps = jnp.concatenate([rows[0, 0, q, pl.ds(first, half), :], rows[0, 0, q, pl.ds(half - first, half), :]], 0)
        done = warp(masked(info, ivar, q) * flux[0, 0, q], maps, cols[0, 0, q])
        send[to, rank] = done[:half]
        send_inner[own * CAP + rank] = done[half:]
    copies = [pltpu.make_async_copy(send.at[d], out, sems.at[d]) for d, out in enumerate(outs)]
    run(copies + [pltpu.make_async_copy(send_inner, inner, sems.at[len(outs)])])


def weight_body(info, *rest):
    *rest, slot_out, acc = rest
    count = slot_out.shape[0] // CAP
    got, out = rest[:count], rest[count:]
    side = acc.shape[1]
    spare = acc.shape[0] - 1
    per_tile = out[0].shape[0]
    slots = []
    for d in range(count):
        for rank in range(CAP):
            at = jnp.max(got[d][rank, side:, :]).astype(jnp.int32)
            slots.append(jnp.where(at < 0, spare, at))
    acc[...] = jnp.zeros(acc.shape, F32)
    for n, at in enumerate(slots):
        d, rank = divmod(n, CAP)
        slot_out[partner(info[ME, 0], d) * CAP + rank] = at
        acc[at] += got[d][rank, :side, :]
    for k in range(len(out)):
        for c in range(per_tile):
            for r in range(BR):
                out[k][c, r * side : (r + 1) * side, :] = acc[r * BC + info[ORDER, k] * per_tile + c]


def outer_body(info, slot, *rest):
    *rest, top, bottom, acc = rest
    count = slot.shape[0] // CAP
    got, tiles = rest[:count], rest[count:]
    half = acc.shape[1]
    per_tile = tiles[0].shape[0]
    acc[...] = jnp.zeros(acc.shape, F32)
    for d in range(count):
        for rank in range(CAP):
            acc[slot[partner(info[ME, 0], d) * CAP + rank]] += got[d][rank]
    for k, tile in enumerate(tiles):
        for c in range(per_tile):
            to = info[ORDER, k] * per_tile + c
            top[to] = acc[to] / jnp.maximum(tile[c, :half, :], 1.0)
            bottom[to] = acc[BC + to] / jnp.maximum(tile[c, -half:, :], 1.0)


def inner_body(info, slot, got, *rest):
    *tiles, image, acc = rest
    half = acc.shape[1]
    per_tile = tiles[0].shape[0]
    acc[...] = jnp.zeros(acc.shape, F32)
    for n in range(slot.shape[0]):
        acc[slot[n]] += got[n]
    for k, tile in enumerate(tiles):
        for c in range(per_tile):
            to = info[ORDER, k] * per_tile + c
            image[to, :half, :] = acc[to] / jnp.maximum(tile[c, half : 2 * half, :], 1.0)
            image[to, half:, :] = acc[BC + to] / jnp.maximum(tile[c, 2 * half : 3 * half, :], 1.0)


def beside(stacked):
    n = stacked.shape[0] // 2
    return jnp.concatenate([stacked[:n], stacked[n:]], 1)


def spectrum_body(coeffs, basis, row_ker, col_fwd, out):
    kernel = coeffs[0, 0] * basis[0]
    for k in range(1, basis.shape[0]):
        kernel = kernel + coeffs[0, k] * basis[k]
    lines = data(beside(dot(row_ker[...], data(kernel, 0))), 1)
    for odd in (0, 1):
        out[odd] = dot(lines, col_fwd[odd])


def conv_body(first, info, above, top, image, bottom, below, spec, row_fwd, col_fwd, col_inv, row_inv, *rest):
    *rest, lines = rest
    count = len(rest) // 2
    weight, out = rest[:count], rest[count:]
    taps = image.shape[2]
    per_tile = weight[0].shape[0]

    def column(c):
        return jnp.concatenate([above[c], top[c], image[c], bottom[c], below[c]], 0)

    def shifted(u):
        if isinstance(u, int):
            gap = jnp.zeros((above.shape[1] * 6, HALO), F32)
            left = column(u - 1)[:, taps - HALO :] if u > 0 else gap
            right = column(u)[:, :HALO] if u < BC else gap
            return jnp.concatenate([left, right], 1)
        left = column(jnp.maximum(u - 1, 0))[:, taps - HALO :]
        right = column(jnp.minimum(u, BC - 1))[:, :HALO]
        left = jnp.where(u > 0, left, 0.0)
        right = jnp.where(u < BC, right, 0.0)
        return jnp.concatenate([left, right], 1)

    one_tile = lines.shape[0] == per_tile + 1
    base = info[ORDER, first] * per_tile if one_tile else 0
    for u in range(0, lines.shape[0], 2):
        n = min(2, lines.shape[0] - u)
        ext = jnp.concatenate([shifted(base + u + i) for i in range(n)], 1)
        got = dot(row_fwd[...], data(ext, 0))
        for i in range(n):
            lines[u + i] = got[:, i * taps : (i + 1) * taps]
    for k in range(count):
        start = 0 if one_tile else info[ORDER, first + k] * per_tile
        one = [lines[start + c] for c in range(per_tile)]
        two = [lines[start + c + 1] for c in range(per_tile)]
        freqs = one[0].shape[0] // 2
        total = []
        for odd in (0, 1):
            mixed = [beside(a - b if odd else a + b) for a, b in zip(one, two)]
            freq = dot(data(jnp.concatenate(mixed, 0), 1), col_fwd[odd])
            kr = jnp.concatenate([spec[odd, :, :taps]] * per_tile, 0)
            ki = jnp.concatenate([spec[odd, :, taps:]] * per_tile, 0)
            zr, zi = freq[:, :taps], freq[:, taps:]
            prod = jnp.concatenate([zr * kr - zi * ki, zr * ki + zi * kr], 1)
            total.append(dot(data(prod, 1), col_inv[odd]))
        wave = total[0] + total[1]
        parts = [wave[c * freqs : (c + 1) * freqs] for c in range(per_tile)]
        cols = [jnp.concatenate([p[:, :taps], p[:, taps:]], 0) for p in parts]
        done = dot(row_inv[...], data(jnp.concatenate(cols, 1), 0))
        for c in range(per_tile):
            out[k][c] = done[:, c * taps : (c + 1) * taps] * weight[k][c]


def total_body(*refs):
    parts, out = refs[:-1], refs[-1]
    side = parts[0].shape[2]
    for c in range(parts[0].shape[0]):
        out[:, c * side : (c + 1) * side] = functools.reduce(jnp.add, [p[c] for p in parts])


def ratio_body(*refs):
    parts, weight, out = refs[:-2], refs[-2], refs[-1]
    side = parts[0].shape[2]
    for c in range(parts[0].shape[0]):
        cols = slice(c * side, (c + 1) * side)
        out[:, cols] = functools.reduce(jnp.add, [p[c] for p in parts]) / jnp.maximum(weight[:, cols], 1.0)


LINE = ((3, 2, 1, 0), (3, 0, 2, 1), (0, 3, 1, 2), (0, 1, 2, 3))


def send_order(count):
    if count == 4:
        return np.array(LINE, np.int32)
    return np.array([list(range(count))] * count, np.int32)


class VisitSum:
    def __init__(self, count):
        self.count = count
        self.sent = []
        self.tiles = []

    def send(self, tile, *routes):
        self.sent += [lax.ppermute(tile, "visit", route) for route in routes]

    def push(self, *tiles):
        for tile in tiles:
            k = len(self.tiles)
            self.tiles.append(tile)
            if self.count == 4:
                if k == 0:
                    self.send(tile, [(0, 1), (3, 2)])
                elif k == 1:
                    self.send(tile, [(0, 2), (1, 0), (2, 3), (3, 1)])
                elif k == 2:
                    self.send(tile, [(0, 1), (1, 2)], [(2, 1), (3, 2)])

    def parts(self):
        if self.count != 4:
            return [lax.psum_scatter(jnp.stack(self.tiles), "visit", scatter_dimension=0, tiled=False)]
        self.send(self.tiles[0] + self.sent[0], [(1, 3), (2, 0)])
        return [self.tiles[3], *self.sent[1:]]


def coadd_patches(piece_flux, piece_ivar, warp_rows, warp_cols, piece_owner, piece_slot, piece_extent, basis, coeffs):
    owners = lax.axis_size("bulk")
    visits = lax.axis_size("visit")
    pieces, side = piece_flux.shape[2:4]
    assert side == LANES and side == 2 * HALO and owners & (owners - 1) == 0
    half = side // 2
    rows_dev = BR * side
    per_tile = BC // visits
    cap = owners * CAP
    row_fwd, row_ker, col_fwd, col_inv, row_inv = [jnp.asarray(t) for t in make_tables(rows_dev, side)]
    freqs = row_fwd.shape[0] // 2
    width = max(pieces, visits)

    def line(values):
        return jnp.pad(values, (0, width - values.shape[0]))

    me = lax.axis_index("bulk").astype(jnp.int32)
    order = jnp.asarray(send_order(visits))[lax.axis_index("visit")]
    info = jnp.stack(
        [
            line(piece_owner[0, 0, :, 0]),
            line(piece_slot[0, 0]),
            line(piece_extent[0, 0, :, 0]),
            line(piece_extent[0, 0, :, 1]),
            jnp.full((width,), me),
            line(order),
        ]
    )

    def arr(*shape):
        return jax.ShapeDtypeStruct(shape, F32)

    hbm = pl.BlockSpec(memory_space=pl.ANY)

    def exchange(sent):
        got = [sent[0]]
        for d in range(1, owners):
            got.append(lax.ppermute(sent[d], "bulk", [(i, i ^ d) for i in range(owners)]))
        return got

    sent_weight = pl.pallas_call(
        warp_weight_body,
        out_shape=[arr(CAP, side + META, side)] * owners,
        in_specs=[SMEM] + [VMEM] * 3,
        out_specs=[hbm] * owners,
        scratch_shapes=[pltpu.VMEM((owners, CAP, side + META, side), F32), pltpu.SemaphoreType.DMA((owners,))],
        name="warp_weight",
    )(info, piece_ivar, warp_rows, warp_cols)
    got_weight = exchange(sent_weight)
    *sent_outer, sent_inner = pl.pallas_call(
        warp_flux_body,
        out_shape=[arr(CAP, half, side)] * owners + [arr(cap, half, side)],
        in_specs=[SMEM] + [VMEM] * 4,
        out_specs=[hbm] * (owners + 1),
        scratch_shapes=[
            pltpu.VMEM((owners, CAP, half, side), F32),
            pltpu.VMEM((cap, half, side), F32),
            pltpu.SemaphoreType.DMA((owners + 1,)),
        ],
        name="warp_flux",
    )(info, piece_flux, piece_ivar, warp_rows, warp_cols)
    got_outer = exchange(sent_outer)
    got_inner = lax.all_to_all(sent_inner, "bulk", split_axis=0, concat_axis=0, tiled=True)
    spec = pl.pallas_call(
        spectrum_body,
        out_shape=arr(2, freqs, 2 * side),
        in_specs=[SMEM] + [VMEM] * 3,
        out_specs=VMEM,
        name="spectrum",
    )(coeffs, basis, row_ker, col_fwd)
    tile = arr(per_tile, rows_dev, side)
    *ivar, slots = pl.pallas_call(
        weight_body,
        out_shape=[tile] * visits + [jax.ShapeDtypeStruct((cap,), jnp.int32)],
        in_specs=[SMEM] + [VMEM] * owners,
        out_specs=[VMEM] * visits + [SMEM],
        scratch_shapes=[pltpu.VMEM((BR * BC + 1, side, side), F32)],
        name="weights",
    )(info, *got_weight)
    weight_sum = VisitSum(visits)
    weight_sum.push(*ivar)
    scratch = [pltpu.VMEM((BR * BC + 1, half, side), F32)]
    top, bottom = pl.pallas_call(
        outer_body,
        out_shape=[arr(BC, half, side)] * 2,
        in_specs=[SMEM] * 2 + [VMEM] * (owners + visits),
        out_specs=[VMEM] * 2,
        scratch_shapes=scratch,
        name="outer",
    )(info, slots, *got_outer, *ivar)
    ends = owners - 1
    above = lax.ppermute(bottom, "bulk", [(i, i + 1) for i in range(ends)])
    below = lax.ppermute(top, "bulk", [(i + 1, i) for i in range(ends)])
    image = pl.pallas_call(
        inner_body,
        out_shape=arr(BC, side, side),
        in_specs=[SMEM] * 2 + [VMEM] * (1 + visits),
        out_specs=VMEM,
        scratch_shapes=scratch,
        name="inner",
    )(info, slots, got_inner, *ivar)
    weight_map = pl.pallas_call(
        total_body, out_shape=arr(rows_dev, per_tile * side), name="weight_map"
    )(*weight_sum.parts())

    def convolve(first, count, blocks):
        return pl.pallas_call(
            functools.partial(conv_body, first),
            out_shape=[tile] * count,
            in_specs=[SMEM] + [VMEM] * (10 + count),
            out_specs=[VMEM] * count,
            scratch_shapes=[pltpu.VMEM((blocks, 2 * freqs, side), F32)],
        )(
            info, above, top, image, bottom, below, spec, row_fwd, col_fwd, col_inv, row_inv,
            *ivar[first : first + count],
        )

    image_sum = VisitSum(visits)
    image_sum.push(*convolve(0, 1, per_tile + 1))
    image_sum.push(*convolve(1, visits - 1, BC + 1))
    coadd = pl.pallas_call(
        ratio_body, out_shape=arr(rows_dev, per_tile * side), name="coadd"
    )(*image_sum.parts(), weight_map)
    return (coadd, weight_map)


def solution(mesh):
    placed = (
        P("visit", "bulk", None, None, None),
        P("visit", "bulk", None, None, None),
        P("visit", "bulk", None, None, None),
        P("visit", "bulk", None, None, None),
        P("visit", "bulk", None, None),
        P("visit", "bulk", None),
        P("visit", "bulk", None, None),
        P(),
        P("visit", None),
    )
    return jax.shard_map(
        coadd_patches,
        mesh=mesh,
        in_specs=placed,
        out_specs=(P("bulk", "visit"), P("bulk", "visit")),
        check_vma=False,
    )
```

```python
import functools
import math

import jax
import jax.numpy as jnp
import numpy as np
from jax import lax
from jax.experimental import pallas as pl
from jax.experimental.pallas import tpu as pltpu
from jax.sharding import PartitionSpec as P


HALO = 64
BR = 2
BC = 8
CAP = 2
LANES = 128
META = 8


F32 = jnp.float32
BF16 = jnp.bfloat16
VMEM = pl.BlockSpec(memory_space=pltpu.VMEM)
SMEM = pl.BlockSpec(memory_space=pltpu.SMEM)


def split(value):
    high = value.astype(BF16)
    low = (value - high.astype(F32)).astype(BF16)
    return high, low


def data(value, axis):
    high, low = split(value)
    return jnp.concatenate([high, low, high], axis)


def weights(value, axis):
    high, low = split(value)
    return jnp.concatenate([high, high, low], axis)


def table(value):
    value = np.asarray(value, np.float32)
    high = value.astype(jnp.bfloat16)
    return np.stack([high, (value - high.astype(np.float32)).astype(jnp.bfloat16)])


def fixed(ref, axis):
    return jnp.concatenate([ref[0], ref[0], ref[1]], axis)


def dot(a, b, dims=((1,), (0,))):
    return lax.dot_general(a, b, (dims, ((), ())), preferred_element_type=F32)


@functools.lru_cache
def make_tables(rows_dev, taps):
    length = rows_dev + taps - 1
    freqs = (length + 1) // 2
    k = np.arange(freqs)[:, None]

    def wave(first, second, period):
        return 2.0 * math.pi * ((first * second) % period) / period

    n = np.arange(rows_dev + 2 * HALO)[None, :] - 1
    theta = wave(k, n, length)
    used = n >= 0
    row_fwd = np.concatenate([np.cos(theta) * used, -np.sin(theta) * used], 0)
    theta = wave(k, np.arange(taps)[None, :], length)
    row_ker = np.concatenate([np.cos(theta), -np.sin(theta)], 0)
    period = 2 * taps
    n = np.arange(taps)[:, None]
    f = np.arange(taps)[None, :]
    col_fwd = []
    col_inv = []
    for odd in (0, 1):
        theta = wave(n, 2 * f + odd, period)
        c, s = np.cos(theta), np.sin(theta)
        col_fwd.append(np.block([[c, -s], [s, c]]))
        c, s = c.T, s.T
        sign = -1.0 if odd else 1.0
        col_inv.append(sign * np.block([[c, s], [-s, c]]))
    p = np.arange(rows_dev)[:, None] + taps - 1
    theta = wave(p, k.T, length)
    weight = np.where(k.T == 0, 1.0, 2.0) / (length * period)
    row_inv = np.concatenate([weight * np.cos(theta), -weight * np.sin(theta)], 1)
    return (
        table(row_fwd),
        table(row_ker),
        np.stack([table(t) for t in col_fwd]),
        np.stack([table(t) for t in col_inv]),
        table(row_inv),
    )


def partner(me, other):
    return jnp.bitwise_xor(me, other)


OWNER, SLOT, ROWS, COLS, ME, ORDER = range(6)


def places(info, pieces):
    for q in range(pieces):
        own = info[OWNER, q]
        rank = jnp.int32(0)
        for earlier in range(q):
            rank = rank + (info[OWNER, earlier] == own).astype(jnp.int32)
        yield q, partner(info[ME, 0], own), own, rank, info[SLOT, q]


def masked(info, ivar, q):
    shape = ivar.shape[3:]
    row_at = lax.broadcasted_iota(jnp.int32, shape, 0)
    col_at = lax.broadcasted_iota(jnp.int32, shape, 1)
    valid = (row_at < info[ROWS, q]) & (col_at < info[COLS, q])
    return jnp.where(valid, ivar[0, 0, q], 0.0)


def warp(plane, rows, cols):
    mid = dot(data(plane, 1), weights(cols, 1), ((1,), (1,)))
    return dot(weights(rows, 1), data(mid, 0))


def run(copies):
    for copy in copies:
        copy.start()
    for copy in copies:
        copy.wait()


def warp_weight_body(info, ivar, rows, cols, *rest):
    pieces, side, _ = ivar.shape[2:]
    *outs, send, sems = rest
    for d in range(len(outs)):
        for rank in range(CAP):
            send[d, rank, side:, :] = jnp.full((META, side), -1.0, F32)
    for q, to, _, rank, at in places(info, pieces):
        send[to, rank, :side, :] = warp(masked(info, ivar, q), rows[0, 0, q], cols[0, 0, q])
        send[to, rank, side:, :] = jnp.full((META, side), at.astype(F32), F32)
    run([pltpu.make_async_copy(send.at[d], out, sems.at[d]) for d, out in enumerate(outs)])


def warp_flux_body(info, flux, ivar, rows, cols, out):
    for q, _, own, rank, _ in places(info, ivar.shape[2]):
        out[own * CAP + rank] = warp(masked(info, ivar, q) * flux[0, 0, q], rows[0, 0, q], cols[0, 0, q])


def weight_body(info, *rest):
    *rest, slot_out, acc = rest
    count = slot_out.shape[0] // CAP
    got, out = rest[:count], rest[count:]
    side = acc.shape[1]
    spare = acc.shape[0] - 1
    per_tile = out[0].shape[0]
    slots = []
    for d in range(count):
        for rank in range(CAP):
            at = jnp.max(got[d][rank, side:, :]).astype(jnp.int32)
            slots.append(jnp.where(at < 0, spare, at))
    acc[...] = jnp.zeros(acc.shape, F32)
    for n, at in enumerate(slots):
        d, rank = divmod(n, CAP)
        slot_out[partner(info[ME, 0], d) * CAP + rank] = at
        acc[at] += got[d][rank, :side, :]
    for k in range(len(out)):
        for c in range(per_tile):
            for r in range(BR):
                out[k][c, r * side : (r + 1) * side, :] = acc[r * BC + info[ORDER, k] * per_tile + c]


def image_body(info, slot, got, *rest):
    *tiles, image, top, bottom, acc = rest
    side = acc.shape[1]
    per_tile = tiles[0].shape[0]
    acc[...] = jnp.zeros(acc.shape, F32)
    for n in range(slot.shape[0]):
        acc[slot[n]] += got[n]
    for k, tile in enumerate(tiles):
        for c in range(per_tile):
            to = info[ORDER, k] * per_tile + c
            for r in range(BR):
                rows = slice(r * side, (r + 1) * side)
                image[to, rows, :] = acc[r * BC + to] / jnp.maximum(tile[c, rows, :], 1.0)
            top[to] = image[to, :HALO, :]
            bottom[to] = image[to, -HALO:, :]


def beside(stacked):
    n = stacked.shape[0] // 2
    return jnp.concatenate([stacked[:n], stacked[n:]], 1)


def spectrum_body(coeffs, basis, row_ker, col_fwd, out):
    kernel = coeffs[0, 0] * basis[0]
    for k in range(1, basis.shape[0]):
        kernel = kernel + coeffs[0, k] * basis[k]
    lines = data(beside(dot(fixed(row_ker, 1), data(kernel, 0))), 1)
    for odd in (0, 1):
        out[odd] = dot(lines, fixed(col_fwd.at[odd], 0))


def conv_body(first, info, above, image, below, spec, row_fwd, col_fwd, col_inv, row_inv, *rest):
    *rest, lines = rest
    count = len(rest) // 2
    weight, out = rest[:count], rest[count:]
    taps = image.shape[2]
    per_tile = weight[0].shape[0]

    def column(c):
        return jnp.concatenate([above[c], image[c], below[c]], 0)

    def shifted(u):
        if isinstance(u, int):
            gap = jnp.zeros((image.shape[1] + 2 * HALO, HALO), F32)
            left = column(u - 1)[:, taps - HALO :] if u > 0 else gap
            right = column(u)[:, :HALO] if u < BC else gap
            return jnp.concatenate([left, right], 1)
        left = column(jnp.maximum(u - 1, 0))[:, taps - HALO :]
        right = column(jnp.minimum(u, BC - 1))[:, :HALO]
        left = jnp.where(u > 0, left, 0.0)
        right = jnp.where(u < BC, right, 0.0)
        return jnp.concatenate([left, right], 1)

    lead = fixed(row_fwd, 1)
    last = fixed(row_inv, 1)
    one_tile = lines.shape[0] == per_tile + 1
    base = info[ORDER, first] * per_tile if one_tile else 0
    for u in range(0, lines.shape[0], 2):
        n = min(2, lines.shape[0] - u)
        ext = jnp.concatenate([shifted(base + u + i) for i in range(n)], 1)
        got = dot(lead, data(ext, 0))
        for i in range(n):
            lines[u + i] = got[:, i * taps : (i + 1) * taps]
    for k in range(count):
        start = 0 if one_tile else info[ORDER, first + k] * per_tile
        one = [lines[start + c] for c in range(per_tile)]
        two = [lines[start + c + 1] for c in range(per_tile)]
        freqs = one[0].shape[0] // 2
        total = []
        for odd in (0, 1):
            mixed = [beside(a - b if odd else a + b) for a, b in zip(one, two)]
            freq = dot(data(jnp.concatenate(mixed, 0), 1), fixed(col_fwd.at[odd], 0))
            kr = jnp.concatenate([spec[odd, :, :taps]] * per_tile, 0)
            ki = jnp.concatenate([spec[odd, :, taps:]] * per_tile, 0)
            zr, zi = freq[:, :taps], freq[:, taps:]
            prod = jnp.concatenate([zr * kr - zi * ki, zr * ki + zi * kr], 1)
            total.append(dot(data(prod, 1), fixed(col_inv.at[odd], 0)))
        wave = total[0] + total[1]
        parts = [wave[c * freqs : (c + 1) * freqs] for c in range(per_tile)]
        cols = [jnp.concatenate([p[:, :taps], p[:, taps:]], 0) for p in parts]
        done = dot(last, data(jnp.concatenate(cols, 1), 0))
        for c in range(per_tile):
            out[k][c] = done[:, c * taps : (c + 1) * taps] * weight[k][c]


def total_body(*refs):
    parts, out = refs[:-1], refs[-1]
    side = parts[0].shape[2]
    for c in range(parts[0].shape[0]):
        out[:, c * side : (c + 1) * side] = functools.reduce(jnp.add, [p[c] for p in parts])


def ratio_body(*refs):
    parts, weight, out = refs[:-2], refs[-2], refs[-1]
    side = parts[0].shape[2]
    for c in range(parts[0].shape[0]):
        cols = slice(c * side, (c + 1) * side)
        out[:, cols] = functools.reduce(jnp.add, [p[c] for p in parts]) / jnp.maximum(weight[:, cols], 1.0)


LINE = ((3, 2, 1, 0), (3, 0, 2, 1), (0, 3, 1, 2), (0, 1, 2, 3))


def send_order(count):
    if count == 4:
        return np.array(LINE, np.int32)
    return np.array([list(range(count))] * count, np.int32)


class VisitSum:
    def __init__(self, count):
        self.count = count
        self.sent = []
        self.tiles = []

    def send(self, tile, *routes):
        self.sent += [lax.ppermute(tile, "visit", route) for route in routes]

    def push(self, *tiles):
        for tile in tiles:
            k = len(self.tiles)
            self.tiles.append(tile)
            if self.count == 4:
                if k == 0:
                    self.send(tile, [(0, 1), (3, 2)])
                elif k == 1:
                    self.send(tile, [(0, 2), (1, 0), (2, 3), (3, 1)])
                elif k == 2:
                    self.send(tile, [(0, 1), (1, 2)], [(2, 1), (3, 2)])

    def parts(self):
        if self.count != 4:
            return [lax.psum_scatter(jnp.stack(self.tiles), "visit", scatter_dimension=0, tiled=False)]
        self.send(self.tiles[0] + self.sent[0], [(1, 3), (2, 0)])
        return [self.tiles[3], *self.sent[1:]]


def coadd_patches(piece_flux, piece_ivar, warp_rows, warp_cols, piece_owner, piece_slot, piece_extent, basis, coeffs):
    owners = lax.axis_size("bulk")
    visits = lax.axis_size("visit")
    pieces, side = piece_flux.shape[2:4]
    assert side == LANES and side == 2 * HALO and owners & (owners - 1) == 0
    rows_dev = BR * side
    per_tile = BC // visits
    cap = owners * CAP
    row_fwd, row_ker, col_fwd, col_inv, row_inv = [jnp.asarray(t) for t in make_tables(rows_dev, side)]
    freqs = row_fwd.shape[1] // 2
    width = max(pieces, visits)

    def line(values):
        return jnp.pad(values, (0, width - values.shape[0]))

    me = lax.axis_index("bulk").astype(jnp.int32)
    order = jnp.asarray(send_order(visits))[lax.axis_index("visit")]
    info = jnp.stack(
        [
            line(piece_owner[0, 0, :, 0]),
            line(piece_slot[0, 0]),
            line(piece_extent[0, 0, :, 0]),
            line(piece_extent[0, 0, :, 1]),
            jnp.full((width,), me),
            line(order),
        ]
    )

    def arr(*shape):
        return jax.ShapeDtypeStruct(shape, F32)

    hbm = pl.BlockSpec(memory_space=pl.ANY)

    def exchange(sent):
        got = [sent[0]]
        for d in range(1, owners):
            got.append(lax.ppermute(sent[d], "bulk", [(i, i ^ d) for i in range(owners)]))
        return got

    sent_weight = pl.pallas_call(
        warp_weight_body,
        out_shape=[arr(CAP, side + META, side)] * owners,
        in_specs=[SMEM] + [VMEM] * 3,
        out_specs=[hbm] * owners,
        scratch_shapes=[pltpu.VMEM((owners, CAP, side + META, side), F32), pltpu.SemaphoreType.DMA((owners,))],
        name="warp_weight",
    )(info, piece_ivar, warp_rows, warp_cols)
    got_weight = exchange(sent_weight)
    sent_flux = pl.pallas_call(
        warp_flux_body,
        out_shape=arr(cap, side, side),
        in_specs=[SMEM] + [VMEM] * 4,
        out_specs=VMEM,
        name="warp_flux",
    )(info, piece_flux, piece_ivar, warp_rows, warp_cols)
    got_flux = lax.all_to_all(sent_flux, "bulk", split_axis=0, concat_axis=0, tiled=True)
    spec = pl.pallas_call(
        spectrum_body,
        out_shape=arr(2, freqs, 2 * side),
        in_specs=[SMEM] + [VMEM] * 3,
        out_specs=VMEM,
        name="spectrum",
    )(coeffs, basis, row_ker, col_fwd)
    tile = arr(per_tile, rows_dev, side)
    *ivar, slots = pl.pallas_call(
        weight_body,
        out_shape=[tile] * visits + [jax.ShapeDtypeStruct((cap,), jnp.int32)],
        in_specs=[SMEM] + [VMEM] * owners,
        out_specs=[VMEM] * visits + [SMEM],
        scratch_shapes=[pltpu.VMEM((BR * BC + 1, side, side), F32)],
        name="weights",
    )(info, *got_weight)
    weight_sum = VisitSum(visits)
    weight_sum.push(*ivar)
    image, top, bottom = pl.pallas_call(
        image_body,
        out_shape=[arr(BC, rows_dev, side)] + [arr(BC, HALO, side)] * 2,
        in_specs=[SMEM] * 2 + [VMEM] * (1 + visits),
        out_specs=[VMEM] * 3,
        scratch_shapes=[pltpu.VMEM((BR * BC + 1, side, side), F32)],
        name="image",
    )(info, slots, got_flux, *ivar)
    ends = owners - 1
    above = lax.ppermute(bottom, "bulk", [(i, i + 1) for i in range(ends)])
    below = lax.ppermute(top, "bulk", [(i + 1, i) for i in range(ends)])
    weight_map = pl.pallas_call(
        total_body, out_shape=arr(rows_dev, per_tile * side), name="weight_map"
    )(*weight_sum.parts())

    def convolve(first, count, blocks):
        return pl.pallas_call(
            functools.partial(conv_body, first),
            out_shape=[tile] * count,
            in_specs=[SMEM] + [VMEM] * (8 + count),
            out_specs=[VMEM] * count,
            scratch_shapes=[pltpu.VMEM((blocks, 2 * freqs, side), F32)],
        )(
            info, above, image, below, spec, row_fwd, col_fwd, col_inv, row_inv,
            *ivar[first : first + count],
        )

    image_sum = VisitSum(visits)
    image_sum.push(*convolve(0, 1, per_tile + 1))
    image_sum.push(*convolve(1, visits - 1, BC + 1))
    coadd = pl.pallas_call(
        ratio_body, out_shape=arr(rows_dev, per_tile * side), name="coadd"
    )(*image_sum.parts(), weight_map)
    return (coadd, weight_map)


def solution(mesh):
    placed = (
        P("visit", "bulk", None, None, None),
        P("visit", "bulk", None, None, None),
        P("visit", "bulk", None, None, None),
        P("visit", "bulk", None, None, None),
        P("visit", "bulk", None, None),
        P("visit", "bulk", None),
        P("visit", "bulk", None, None),
        P(),
        P("visit", None),
    )
    return jax.shard_map(
        coadd_patches,
        mesh=mesh,
        in_specs=placed,
        out_specs=(P("bulk", "visit"), P("bulk", "visit")),
        check_vma=False,
    )
```

```python
import functools
import math

import jax
import jax.numpy as jnp
import numpy as np
from jax import lax
from jax.experimental import pallas as pl
from jax.experimental.pallas import tpu as pltpu
from jax.sharding import PartitionSpec as P


HALO = 64
BR = 2
BC = 8
CAP = 2
LANES = 128
VMEM_BYTES = 12 * 2**20
META = 8


F32 = jnp.float32
BF16 = jnp.bfloat16
VMEM = pl.BlockSpec(memory_space=pltpu.VMEM)
SMEM = pl.BlockSpec(memory_space=pltpu.SMEM)


def split(value):
    high = value.astype(BF16)
    low = (value - high.astype(F32)).astype(BF16)
    return high, low


def data(value, axis):
    high, low = split(value)
    return jnp.concatenate([high, low, high], axis)


def weights(value, axis):
    high, low = split(value)
    return jnp.concatenate([high, high, low], axis)


def table(value):
    value = np.asarray(value, np.float32)
    high = value.astype(jnp.bfloat16)
    return np.stack([high, (value - high.astype(np.float32)).astype(jnp.bfloat16)])


def fixed(ref, axis):
    return jnp.concatenate([ref[0], ref[0], ref[1]], axis)


def dot(a, b, dims=((1,), (0,))):
    return lax.dot_general(a, b, (dims, ((), ())), preferred_element_type=F32)


@functools.lru_cache
def make_tables(rows_dev, taps):
    length = rows_dev + taps - 1
    freqs = (length + 1) // 2
    k = np.arange(freqs)[:, None]

    def wave(first, second, period):
        return 2.0 * math.pi * ((first * second) % period) / period

    n = np.arange(rows_dev + 2 * HALO)[None, :] - 1
    theta = wave(k, n, length)
    used = n >= 0
    row_fwd = np.concatenate([np.cos(theta) * used, -np.sin(theta) * used], 0)
    theta = wave(k, np.arange(taps)[None, :], length)
    row_ker = np.concatenate([np.cos(theta), -np.sin(theta)], 0)
    period = 2 * taps
    n = np.arange(taps)[:, None]
    f = np.arange(taps)[None, :]
    col_fwd = []
    col_inv = []
    for odd in (0, 1):
        theta = wave(n, 2 * f + odd, period)
        c, s = np.cos(theta), np.sin(theta)
        col_fwd.append(np.block([[c, -s], [s, c]]))
        c, s = c.T, s.T
        sign = -1.0 if odd else 1.0
        col_inv.append(sign * np.block([[c, s], [-s, c]]))
    p = np.arange(rows_dev)[:, None] + taps - 1
    theta = wave(p, k.T, length)
    weight = np.where(k.T == 0, 1.0, 2.0) / (length * period)
    row_inv = np.concatenate([weight * np.cos(theta), -weight * np.sin(theta)], 1)
    return (
        table(row_fwd),
        table(row_ker),
        np.stack([table(t) for t in col_fwd]),
        np.stack([table(t) for t in col_inv]),
        table(row_inv),
    )


def partner(me, other):
    return jnp.bitwise_xor(me, other)


OWNER, SLOT, ROWS, COLS, ME, ORDER = range(6)


def places(info, pieces):
    for q in range(pieces):
        own = info[OWNER, q]
        rank = jnp.int32(0)
        for earlier in range(q):
            rank = rank + (info[OWNER, earlier] == own).astype(jnp.int32)
        yield q, partner(info[ME, 0], own), own, rank, info[SLOT, q]


def masked(info, ivar, q):
    shape = ivar.shape[3:]
    row_at = lax.broadcasted_iota(jnp.int32, shape, 0)
    col_at = lax.broadcasted_iota(jnp.int32, shape, 1)
    valid = (row_at < info[ROWS, q]) & (col_at < info[COLS, q])
    return jnp.where(valid, ivar[0, 0, q], 0.0)


def warp(plane, rows, cols):
    mid = dot(data(plane, 1), weights(cols, 1), ((1,), (1,)))
    return dot(weights(rows, 1), data(mid, 0))


def run(copies):
    for copy in copies:
        copy.start()
    for copy in copies:
        copy.wait()


def warp_weight_body(info, ivar, rows, cols, *rest):
    pieces, side, _ = ivar.shape[2:]
    *outs, send, sems = rest
    for d in range(len(outs)):
        for rank in range(CAP):
            send[d, rank, side:, :] = jnp.full((META, side), -1.0, F32)
    for q, to, _, rank, at in places(info, pieces):
        send[to, rank, :side, :] = warp(masked(info, ivar, q), rows[0, 0, q], cols[0, 0, q])
        send[to, rank, side:, :] = jnp.full((META, side), at.astype(F32), F32)
    run([pltpu.make_async_copy(send.at[d], out, sems.at[d]) for d, out in enumerate(outs)])


def warp_flux_body(info, flux, ivar, rows, cols, out):
    for q, _, own, rank, _ in places(info, ivar.shape[2]):
        out[own * CAP + rank] = warp(masked(info, ivar, q) * flux[0, 0, q], rows[0, 0, q], cols[0, 0, q])


def weight_body(info, *rest):
    *rest, slot_out, acc = rest
    count = slot_out.shape[0] // CAP
    got, out = rest[:count], rest[count:]
    side = acc.shape[1]
    spare = acc.shape[0] - 1
    per_tile = out[0].shape[0]
    slots = []
    for d in range(count):
        for rank in range(CAP):
            at = jnp.max(got[d][rank, side:, :]).astype(jnp.int32)
            slots.append(jnp.where(at < 0, spare, at))
    acc[...] = jnp.zeros(acc.shape, F32)
    for n, at in enumerate(slots):
        d, rank = divmod(n, CAP)
        slot_out[partner(info[ME, 0], d) * CAP + rank] = at
        acc[at] += got[d][rank, :side, :]
    for k in range(len(out)):
        for c in range(per_tile):
            for r in range(BR):
                out[k][c, r * side : (r + 1) * side, :] = acc[r * BC + info[ORDER, k] * per_tile + c]


def image_body(info, slot, got, *rest):
    *tiles, image, top, bottom, acc = rest
    side = acc.shape[1]
    per_tile = tiles[0].shape[0]
    acc[...] = jnp.zeros(acc.shape, F32)
    for n in range(slot.shape[0]):
        acc[slot[n]] += got[n]
    for k, tile in enumerate(tiles):
        for c in range(per_tile):
            to = info[ORDER, k] * per_tile + c
            for r in range(BR):
                rows = slice(r * side, (r + 1) * side)
                image[to, rows, :] = acc[r * BC + to] / jnp.maximum(tile[c, rows, :], 1.0)
            top[to] = image[to, :HALO, :]
            bottom[to] = image[to, -HALO:, :]


def beside(stacked):
    n = stacked.shape[0] // 2
    return jnp.concatenate([stacked[:n], stacked[n:]], 1)


def spectrum_body(coeffs, basis, row_ker, col_fwd, out):
    kernel = coeffs[0, 0] * basis[0]
    for k in range(1, basis.shape[0]):
        kernel = kernel + coeffs[0, k] * basis[k]
    lines = data(beside(dot(fixed(row_ker, 1), data(kernel, 0))), 1)
    for odd in (0, 1):
        out[odd] = dot(lines, fixed(col_fwd.at[odd], 0))


def conv_body(first, info, above, image, below, spec, row_fwd, col_fwd, col_inv, row_inv, *rest):
    *rest, lines = rest
    count = len(rest) // 2
    weight, out = rest[:count], rest[count:]
    taps = image.shape[2]
    per_tile = weight[0].shape[0]

    def column(c):
        return jnp.concatenate([above[c], image[c], below[c]], 0)

    def shifted(u):
        if isinstance(u, int):
            gap = jnp.zeros((image.shape[1] + 2 * HALO, HALO), F32)
            left = column(u - 1)[:, taps - HALO :] if u > 0 else gap
            right = column(u)[:, :HALO] if u < BC else gap
            return jnp.concatenate([left, right], 1)
        left = column(jnp.maximum(u - 1, 0))[:, taps - HALO :]
        right = column(jnp.minimum(u, BC - 1))[:, :HALO]
        left = jnp.where(u > 0, left, 0.0)
        right = jnp.where(u < BC, right, 0.0)
        return jnp.concatenate([left, right], 1)

    lead = fixed(row_fwd, 1)
    last = fixed(row_inv, 1)
    one_tile = lines.shape[0] == per_tile + 1
    base = info[ORDER, first] * per_tile if one_tile else 0
    for u in range(0, lines.shape[0], 2):
        n = min(2, lines.shape[0] - u)
        ext = jnp.concatenate([shifted(base + u + i) for i in range(n)], 1)
        got = dot(lead, data(ext, 0))
        for i in range(n):
            lines[u + i] = got[:, i * taps : (i + 1) * taps]
    for k in range(count):
        start = 0 if one_tile else info[ORDER, first + k] * per_tile
        one = [lines[start + c] for c in range(per_tile)]
        two = [lines[start + c + 1] for c in range(per_tile)]
        freqs = one[0].shape[0] // 2
        total = []
        for odd in (0, 1):
            mixed = [beside(a - b if odd else a + b) for a, b in zip(one, two)]
            freq = dot(data(jnp.concatenate(mixed, 0), 1), fixed(col_fwd.at[odd], 0))
            kr = jnp.concatenate([spec[odd, :, :taps]] * per_tile, 0)
            ki = jnp.concatenate([spec[odd, :, taps:]] * per_tile, 0)
            zr, zi = freq[:, :taps], freq[:, taps:]
            prod = jnp.concatenate([zr * kr - zi * ki, zr * ki + zi * kr], 1)
            total.append(dot(data(prod, 1), fixed(col_inv.at[odd], 0)))
        wave = total[0] + total[1]
        parts = [wave[c * freqs : (c + 1) * freqs] for c in range(per_tile)]
        cols = [jnp.concatenate([p[:, :taps], p[:, taps:]], 0) for p in parts]
        done = dot(last, data(jnp.concatenate(cols, 1), 0))
        for c in range(per_tile):
            out[k][c] = done[:, c * taps : (c + 1) * taps] * weight[k][c]


def total_body(*refs):
    parts, out = refs[:-1], refs[-1]
    side = parts[0].shape[2]
    for c in range(parts[0].shape[0]):
        out[:, c * side : (c + 1) * side] = functools.reduce(jnp.add, [p[c] for p in parts])


def ratio_body(*refs):
    parts, weight, out = refs[:-2], refs[-2], refs[-1]
    side = parts[0].shape[2]
    for c in range(parts[0].shape[0]):
        cols = slice(c * side, (c + 1) * side)
        out[:, cols] = functools.reduce(jnp.add, [p[c] for p in parts]) / jnp.maximum(weight[:, cols], 1.0)


LINE = ((3, 2, 1, 0), (3, 0, 2, 1), (0, 3, 1, 2), (0, 1, 2, 3))


def send_order(count):
    if count == 4:
        return np.array(LINE, np.int32)
    return np.array([list(range(count))] * count, np.int32)


class VisitSum:
    def __init__(self, count):
        self.count = count
        self.sent = []
        self.tiles = []

    def send(self, tile, *routes):
        self.sent += [lax.ppermute(tile, "visit", route) for route in routes]

    def push(self, *tiles):
        for tile in tiles:
            k = len(self.tiles)
            self.tiles.append(tile)
            if self.count == 4:
                if k == 0:
                    self.send(tile, [(0, 1), (3, 2)])
                elif k == 1:
                    self.send(tile, [(0, 2), (1, 0), (2, 3), (3, 1)])
                elif k == 2:
                    self.send(tile, [(0, 1), (1, 2)], [(2, 1), (3, 2)])

    def parts(self):
        if self.count != 4:
            return [lax.psum_scatter(jnp.stack(self.tiles), "visit", scatter_dimension=0, tiled=False)]
        self.send(self.tiles[0] + self.sent[0], [(1, 3), (2, 0)])
        return [self.tiles[3], *self.sent[1:]]


def coadd_patches(piece_flux, piece_ivar, warp_rows, warp_cols, piece_owner, piece_slot, piece_extent, basis, coeffs):
    owners = lax.axis_size("bulk")
    visits = lax.axis_size("visit")
    pieces, side = piece_flux.shape[2:4]
    assert side == LANES and side == 2 * HALO and owners & (owners - 1) == 0
    rows_dev = BR * side
    per_tile = BC // visits
    cap = owners * CAP
    row_fwd, row_ker, col_fwd, col_inv, row_inv = [jnp.asarray(t) for t in make_tables(rows_dev, side)]
    freqs = row_fwd.shape[1] // 2
    width = max(pieces, visits)

    def line(values):
        return jnp.pad(values, (0, width - values.shape[0]))

    me = lax.axis_index("bulk").astype(jnp.int32)
    order = jnp.asarray(send_order(visits))[lax.axis_index("visit")]
    info = jnp.stack(
        [
            line(piece_owner[0, 0, :, 0]),
            line(piece_slot[0, 0]),
            line(piece_extent[0, 0, :, 0]),
            line(piece_extent[0, 0, :, 1]),
            jnp.full((width,), me),
            line(order),
        ]
    )

    params = pltpu.CompilerParams(vmem_limit_bytes=VMEM_BYTES)

    def arr(*shape):
        return jax.ShapeDtypeStruct(shape, F32)

    hbm = pl.BlockSpec(memory_space=pl.ANY)

    def exchange(sent):
        got = [sent[0]]
        for d in range(1, owners):
            got.append(lax.ppermute(sent[d], "bulk", [(i, i ^ d) for i in range(owners)]))
        return got

    sent_weight = pl.pallas_call(
        warp_weight_body,
        out_shape=[arr(CAP, side + META, side)] * owners,
        in_specs=[SMEM] + [VMEM] * 3,
        out_specs=[hbm] * owners,
        scratch_shapes=[pltpu.VMEM((owners, CAP, side + META, side), F32), pltpu.SemaphoreType.DMA((owners,))],
        compiler_params=params,
        name="warp_weight",
    )(info, piece_ivar, warp_rows, warp_cols)
    got_weight = exchange(sent_weight)
    sent_flux = pl.pallas_call(
        warp_flux_body,
        out_shape=arr(cap, side, side),
        in_specs=[SMEM] + [VMEM] * 4,
        out_specs=VMEM,
        compiler_params=params,
        name="warp_flux",
    )(info, piece_flux, piece_ivar, warp_rows, warp_cols)
    got_flux = lax.all_to_all(sent_flux, "bulk", split_axis=0, concat_axis=0, tiled=True)
    spec = pl.pallas_call(
        spectrum_body,
        out_shape=arr(2, freqs, 2 * side),
        in_specs=[SMEM] + [VMEM] * 3,
        out_specs=VMEM,
        compiler_params=params,
        name="spectrum",
    )(coeffs, basis, row_ker, col_fwd)
    tile = arr(per_tile, rows_dev, side)
    *ivar, slots = pl.pallas_call(
        weight_body,
        out_shape=[tile] * visits + [jax.ShapeDtypeStruct((cap,), jnp.int32)],
        in_specs=[SMEM] + [VMEM] * owners,
        out_specs=[VMEM] * visits + [SMEM],
        scratch_shapes=[pltpu.VMEM((BR * BC + 1, side, side), F32)],
        compiler_params=params,
        name="weights",
    )(info, *got_weight)
    weight_sum = VisitSum(visits)
    weight_sum.push(*ivar)
    image, top, bottom = pl.pallas_call(
        image_body,
        out_shape=[arr(BC, rows_dev, side)] + [arr(BC, HALO, side)] * 2,
        in_specs=[SMEM] * 2 + [VMEM] * (1 + visits),
        out_specs=[VMEM] * 3,
        scratch_shapes=[pltpu.VMEM((BR * BC + 1, side, side), F32)],
        compiler_params=params,
        name="image",
    )(info, slots, got_flux, *ivar)
    ends = owners - 1
    above = lax.ppermute(bottom, "bulk", [(i, i + 1) for i in range(ends)])
    below = lax.ppermute(top, "bulk", [(i + 1, i) for i in range(ends)])
    weight_map = pl.pallas_call(
        total_body, out_shape=arr(rows_dev, per_tile * side), compiler_params=params, name="weight_map"
    )(*weight_sum.parts())

    def convolve(first, count, blocks):
        return pl.pallas_call(
            functools.partial(conv_body, first),
            out_shape=[tile] * count,
            in_specs=[SMEM] + [VMEM] * (8 + count),
            out_specs=[VMEM] * count,
            scratch_shapes=[pltpu.VMEM((blocks, 2 * freqs, side), F32)],
            compiler_params=params,
        )(
            info, above, image, below, spec, row_fwd, col_fwd, col_inv, row_inv,
            *ivar[first : first + count],
        )

    image_sum = VisitSum(visits)
    image_sum.push(*convolve(0, 1, per_tile + 1))
    image_sum.push(*convolve(1, visits - 1, BC + 1))
    coadd = pl.pallas_call(
        ratio_body, out_shape=arr(rows_dev, per_tile * side), compiler_params=params, name="coadd"
    )(*image_sum.parts(), weight_map)
    return (coadd, weight_map)


def solution(mesh):
    placed = (
        P("visit", "bulk", None, None, None),
        P("visit", "bulk", None, None, None),
        P("visit", "bulk", None, None, None),
        P("visit", "bulk", None, None, None),
        P("visit", "bulk", None, None),
        P("visit", "bulk", None),
        P("visit", "bulk", None, None),
        P(),
        P("visit", None),
    )
    return jax.shard_map(
        coadd_patches,
        mesh=mesh,
        in_specs=placed,
        out_specs=(P("bulk", "visit"), P("bulk", "visit")),
        check_vma=False,
    )
```

```python
import functools
import math

import jax
import jax.numpy as jnp
import numpy as np
from jax import lax
from jax.experimental import pallas as pl
from jax.experimental.pallas import tpu as pltpu
from jax.sharding import PartitionSpec as P


HALO = 64
BR = 2
BC = 8
CAP = 2
LANES = 128
VMEM_BYTES = 12 * 2**20
META = 8


F32 = jnp.float32
BF16 = jnp.bfloat16
VMEM = pl.BlockSpec(memory_space=pltpu.VMEM)
SMEM = pl.BlockSpec(memory_space=pltpu.SMEM)


def split(value):
    high = value.astype(BF16)
    low = (value - high.astype(F32)).astype(BF16)
    return high, low


def data(value, axis):
    high, low = split(value)
    return jnp.concatenate([high, low, high], axis)


def weights(value, axis):
    high, low = split(value)
    return jnp.concatenate([high, high, low], axis)


def table(value):
    value = np.asarray(value, np.float32)
    high = value.astype(jnp.bfloat16)
    return np.stack([high, (value - high.astype(np.float32)).astype(jnp.bfloat16)])


def fixed(ref, axis):
    return jnp.concatenate([ref[0], ref[0], ref[1]], axis)


def dot(a, b, dims=((1,), (0,))):
    return lax.dot_general(a, b, (dims, ((), ())), preferred_element_type=F32)


@functools.lru_cache
def make_tables(rows_dev, taps):
    length = rows_dev + taps - 1
    freqs = (length + 1) // 2
    k = np.arange(freqs)[:, None]

    def wave(first, second, period):
        return 2.0 * math.pi * ((first * second) % period) / period

    n = np.arange(rows_dev + 2 * HALO)[None, :] - 1
    theta = wave(k, n, length)
    used = n >= 0
    row_fwd = np.concatenate([np.cos(theta) * used, -np.sin(theta) * used], 0)
    theta = wave(k, np.arange(taps)[None, :], length)
    row_ker = np.concatenate([np.cos(theta), -np.sin(theta)], 0)
    period = 2 * taps
    n = np.arange(taps)[:, None]
    f = np.arange(taps)[None, :]
    col_fwd = []
    col_inv = []
    for odd in (0, 1):
        theta = wave(n, 2 * f + odd, period)
        c, s = np.cos(theta), np.sin(theta)
        col_fwd.append(np.block([[c, -s], [s, c]]))
        c, s = c.T, s.T
        sign = -1.0 if odd else 1.0
        col_inv.append(sign * np.block([[c, s], [-s, c]]))
    p = np.arange(rows_dev)[:, None] + taps - 1
    theta = wave(p, k.T, length)
    weight = np.where(k.T == 0, 1.0, 2.0) / (length * period)
    row_inv = np.concatenate([weight * np.cos(theta), -weight * np.sin(theta)], 1)
    return (
        table(row_fwd),
        table(row_ker),
        np.stack([table(t) for t in col_fwd]),
        np.stack([table(t) for t in col_inv]),
        table(row_inv),
    )


def partner(me, other):
    return jnp.bitwise_xor(me, other)


OWNER, SLOT, ROWS, COLS, ME, ORDER = range(6)


def places(info, pieces):
    for q in range(pieces):
        own = info[OWNER, q]
        rank = jnp.int32(0)
        for earlier in range(q):
            rank = rank + (info[OWNER, earlier] == own).astype(jnp.int32)
        yield q, partner(info[ME, 0], own), own, rank, info[SLOT, q]


def masked(info, ivar, q):
    shape = ivar.shape[3:]
    row_at = lax.broadcasted_iota(jnp.int32, shape, 0)
    col_at = lax.broadcasted_iota(jnp.int32, shape, 1)
    valid = (row_at < info[ROWS, q]) & (col_at < info[COLS, q])
    return jnp.where(valid, ivar[0, 0, q], 0.0)


def warp(plane, rows, cols):
    mid = dot(data(plane, 1), weights(cols, 1), ((1,), (1,)))
    return dot(weights(rows, 1), data(mid, 0))


def run(copies):
    for copy in copies:
        copy.start()
    for copy in copies:
        copy.wait()


def warp_weight_body(info, ivar, rows, cols, *rest):
    pieces, side, _ = ivar.shape[2:]
    *outs, send, sems = rest
    for d in range(len(outs)):
        for rank in range(CAP):
            send[d, rank, side:, :] = jnp.full((META, side), -1.0, F32)
    for q, to, _, rank, at in places(info, pieces):
        send[to, rank, :side, :] = warp(masked(info, ivar, q), rows[0, 0, q], cols[0, 0, q])
        send[to, rank, side:, :] = jnp.full((META, side), at.astype(F32), F32)
    run([pltpu.make_async_copy(send.at[d], out, sems.at[d]) for d, out in enumerate(outs)])


def warp_flux_body(info, flux, ivar, rows, cols, out):
    for q, _, own, rank, _ in places(info, ivar.shape[2]):
        out[own * CAP + rank] = warp(masked(info, ivar, q) * flux[0, 0, q], rows[0, 0, q], cols[0, 0, q])


def weight_body(info, *rest):
    *rest, slot_out, acc = rest
    count = slot_out.shape[0] // CAP
    got, out = rest[:count], rest[count:]
    side = acc.shape[1]
    spare = acc.shape[0] - 1
    per_tile = out[0].shape[0]
    slots = []
    for d in range(count):
        for rank in range(CAP):
            at = jnp.max(got[d][rank, side:, :]).astype(jnp.int32)
            slots.append(jnp.where(at < 0, spare, at))
    acc[...] = jnp.zeros(acc.shape, F32)
    for n, at in enumerate(slots):
        d, rank = divmod(n, CAP)
        slot_out[partner(info[ME, 0], d) * CAP + rank] = at
        acc[at] += got[d][rank, :side, :]
    for k in range(len(out)):
        for c in range(per_tile):
            for r in range(BR):
                out[k][c, r * side : (r + 1) * side, :] = acc[r * BC + info[ORDER, k] * per_tile + c]


def image_body(info, slot, got, *rest):
    *tiles, image, top, bottom, acc = rest
    side = acc.shape[1]
    per_tile = tiles[0].shape[0]
    acc[...] = jnp.zeros(acc.shape, F32)
    for n in range(slot.shape[0]):
        acc[slot[n]] += got[n]
    for k, tile in enumerate(tiles):
        for c in range(per_tile):
            to = info[ORDER, k] * per_tile + c
            for r in range(BR):
                rows = slice(r * side, (r + 1) * side)
                image[to, rows, :] = acc[r * BC + to] / jnp.maximum(tile[c, rows, :], 1.0)
            top[to] = image[to, :HALO, :]
            bottom[to] = image[to, -HALO:, :]


def beside(stacked):
    n = stacked.shape[0] // 2
    return jnp.concatenate([stacked[:n], stacked[n:]], 1)


def spectrum_body(coeffs, basis, row_ker, col_fwd, out):
    kernel = coeffs[0, 0] * basis[0]
    for k in range(1, basis.shape[0]):
        kernel = kernel + coeffs[0, k] * basis[k]
    lines = data(beside(dot(fixed(row_ker, 1), data(kernel, 0))), 1)
    for odd in (0, 1):
        out[odd] = dot(lines, fixed(col_fwd.at[odd], 0))


def conv_body(first, info, above, image, below, spec, row_fwd, col_fwd, col_inv, row_inv, *rest):
    *rest, lines = rest
    count = len(rest) // 2
    weight, out = rest[:count], rest[count:]
    taps = image.shape[2]
    per_tile = weight[0].shape[0]

    def column(c):
        return jnp.concatenate([above[c], image[c], below[c]], 0)

    def shifted(u):
        if isinstance(u, int):
            gap = jnp.zeros((image.shape[1] + 2 * HALO, HALO), F32)
            left = column(u - 1)[:, taps - HALO :] if u > 0 else gap
            right = column(u)[:, :HALO] if u < BC else gap
            return jnp.concatenate([left, right], 1)
        left = column(jnp.maximum(u - 1, 0))[:, taps - HALO :]
        right = column(jnp.minimum(u, BC - 1))[:, :HALO]
        left = jnp.where(u > 0, left, 0.0)
        right = jnp.where(u < BC, right, 0.0)
        return jnp.concatenate([left, right], 1)

    lead = fixed(row_fwd, 1)
    last = fixed(row_inv, 1)
    one_tile = lines.shape[0] == per_tile + 1
    base = info[ORDER, first] * per_tile if one_tile else 0
    for u in range(0, lines.shape[0], 2):
        n = min(2, lines.shape[0] - u)
        ext = jnp.concatenate([shifted(base + u + i) for i in range(n)], 1)
        got = dot(lead, data(ext, 0))
        for i in range(n):
            lines[u + i] = got[:, i * taps : (i + 1) * taps]
    for k in range(count):
        start = 0 if one_tile else info[ORDER, first + k] * per_tile
        one = [lines[start + c] for c in range(per_tile)]
        two = [lines[start + c + 1] for c in range(per_tile)]
        freqs = one[0].shape[0] // 2
        total = []
        for odd in (0, 1):
            mixed = [beside(a - b if odd else a + b) for a, b in zip(one, two)]
            freq = dot(data(jnp.concatenate(mixed, 0), 1), fixed(col_fwd.at[odd], 0))
            kr = jnp.concatenate([spec[odd, :, :taps]] * per_tile, 0)
            ki = jnp.concatenate([spec[odd, :, taps:]] * per_tile, 0)
            zr, zi = freq[:, :taps], freq[:, taps:]
            prod = jnp.concatenate([zr * kr - zi * ki, zr * ki + zi * kr], 1)
            total.append(dot(data(prod, 1), fixed(col_inv.at[odd], 0)))
        wave = total[0] + total[1]
        parts = [wave[c * freqs : (c + 1) * freqs] for c in range(per_tile)]
        cols = [jnp.concatenate([p[:, :taps], p[:, taps:]], 0) for p in parts]
        done = dot(last, data(jnp.concatenate(cols, 1), 0))
        for c in range(per_tile):
            out[k][c] = done[:, c * taps : (c + 1) * taps] * weight[k][c]


def total_body(*refs):
    parts, out = refs[:-1], refs[-1]
    side = parts[0].shape[2]
    for c in range(parts[0].shape[0]):
        out[:, c * side : (c + 1) * side] = functools.reduce(jnp.add, [p[c] for p in parts])


def ratio_body(*refs):
    parts, weight, out = refs[:-2], refs[-2], refs[-1]
    side = parts[0].shape[2]
    for c in range(parts[0].shape[0]):
        cols = slice(c * side, (c + 1) * side)
        out[:, cols] = functools.reduce(jnp.add, [p[c] for p in parts]) / jnp.maximum(weight[:, cols], 1.0)


LINE = ((3, 2, 1, 0), (2, 3, 0, 1), (1, 0, 3, 2), (0, 1, 2, 3))


def send_order(count):
    if count == 4:
        return np.array(LINE, np.int32)
    return np.array([list(range(count))] * count, np.int32)


class VisitSum:
    def __init__(self, count):
        self.count = count
        self.sent = []
        self.tiles = []

    def send(self, tile, *routes):
        self.sent += [lax.ppermute(tile, "visit", route) for route in routes]

    def push(self, *tiles):
        for tile in tiles:
            k = len(self.tiles)
            self.tiles.append(tile)
            if self.count != 4:
                continue
            if k == 0:
                self.send(tile, [(0, 1), (3, 2)])
                self.send(tile, [(1, 2), (2, 1)])
            elif k == 1:
                self.send(tile + self.sent[0], [(0, 2), (1, 3), (2, 0), (3, 1)])
            elif k == 2:
                self.send(tile, [(0, 1), (1, 0), (2, 3), (3, 2)])

    def parts(self):
        if self.count != 4:
            return [lax.psum_scatter(jnp.stack(self.tiles), "visit", scatter_dimension=0, tiled=False)]
        return [self.tiles[3], *self.sent[1:]]


def coadd_patches(piece_flux, piece_ivar, warp_rows, warp_cols, piece_owner, piece_slot, piece_extent, basis, coeffs):
    owners = lax.axis_size("bulk")
    visits = lax.axis_size("visit")
    pieces, side = piece_flux.shape[2:4]
    assert side == LANES and side == 2 * HALO and owners & (owners - 1) == 0
    rows_dev = BR * side
    per_tile = BC // visits
    cap = owners * CAP
    row_fwd, row_ker, col_fwd, col_inv, row_inv = [jnp.asarray(t) for t in make_tables(rows_dev, side)]
    freqs = row_fwd.shape[1] // 2
    width = max(pieces, visits)

    def line(values):
        return jnp.pad(values, (0, width - values.shape[0]))

    me = lax.axis_index("bulk").astype(jnp.int32)
    order = jnp.asarray(send_order(visits))[lax.axis_index("visit")]
    info = jnp.stack(
        [
            line(piece_owner[0, 0, :, 0]),
            line(piece_slot[0, 0]),
            line(piece_extent[0, 0, :, 0]),
            line(piece_extent[0, 0, :, 1]),
            jnp.full((width,), me),
            line(order),
        ]
    )

    params = pltpu.CompilerParams(vmem_limit_bytes=VMEM_BYTES)

    def arr(*shape):
        return jax.ShapeDtypeStruct(shape, F32)

    hbm = pl.BlockSpec(memory_space=pl.ANY)

    def exchange(sent):
        got = [sent[0]]
        for d in range(1, owners):
            got.append(lax.ppermute(sent[d], "bulk", [(i, i ^ d) for i in range(owners)]))
        return got

    sent_weight = pl.pallas_call(
        warp_weight_body,
        out_shape=[arr(CAP, side + META, side)] * owners,
        in_specs=[SMEM] + [VMEM] * 3,
        out_specs=[hbm] * owners,
        scratch_shapes=[pltpu.VMEM((owners, CAP, side + META, side), F32), pltpu.SemaphoreType.DMA((owners,))],
        compiler_params=params,
        name="warp_weight",
    )(info, piece_ivar, warp_rows, warp_cols)
    got_weight = exchange(sent_weight)
    sent_flux = pl.pallas_call(
        warp_flux_body,
        out_shape=arr(cap, side, side),
        in_specs=[SMEM] + [VMEM] * 4,
        out_specs=VMEM,
        compiler_params=params,
        name="warp_flux",
    )(info, piece_flux, piece_ivar, warp_rows, warp_cols)
    got_flux = lax.all_to_all(sent_flux, "bulk", split_axis=0, concat_axis=0, tiled=True)
    spec = pl.pallas_call(
        spectrum_body,
        out_shape=arr(2, freqs, 2 * side),
        in_specs=[SMEM] + [VMEM] * 3,
        out_specs=VMEM,
        compiler_params=params,
        name="spectrum",
    )(coeffs, basis, row_ker, col_fwd)
    tile = arr(per_tile, rows_dev, side)
    *ivar, slots = pl.pallas_call(
        weight_body,
        out_shape=[tile] * visits + [jax.ShapeDtypeStruct((cap,), jnp.int32)],
        in_specs=[SMEM] + [VMEM] * owners,
        out_specs=[VMEM] * visits + [SMEM],
        scratch_shapes=[pltpu.VMEM((BR * BC + 1, side, side), F32)],
        compiler_params=params,
        name="weights",
    )(info, *got_weight)
    weight_sum = VisitSum(visits)
    weight_sum.push(*ivar)
    image, top, bottom = pl.pallas_call(
        image_body,
        out_shape=[arr(BC, rows_dev, side)] + [arr(BC, HALO, side)] * 2,
        in_specs=[SMEM] * 2 + [VMEM] * (1 + visits),
        out_specs=[VMEM] * 3,
        scratch_shapes=[pltpu.VMEM((BR * BC + 1, side, side), F32)],
        compiler_params=params,
        name="image",
    )(info, slots, got_flux, *ivar)
    ends = owners - 1
    above = lax.ppermute(bottom, "bulk", [(i, i + 1) for i in range(ends)])
    below = lax.ppermute(top, "bulk", [(i + 1, i) for i in range(ends)])
    weight_map = pl.pallas_call(
        total_body, out_shape=arr(rows_dev, per_tile * side), compiler_params=params, name="weight_map"
    )(*weight_sum.parts())

    def convolve(first, count, blocks):
        return pl.pallas_call(
            functools.partial(conv_body, first),
            out_shape=[tile] * count,
            in_specs=[SMEM] + [VMEM] * (8 + count),
            out_specs=[VMEM] * count,
            scratch_shapes=[pltpu.VMEM((blocks, 2 * freqs, side), F32)],
            compiler_params=params,
        )(
            info, above, image, below, spec, row_fwd, col_fwd, col_inv, row_inv,
            *ivar[first : first + count],
        )

    image_sum = VisitSum(visits)
    image_sum.push(*convolve(0, 1, per_tile + 1))
    image_sum.push(*convolve(1, visits - 1, BC + 1))
    coadd = pl.pallas_call(
        ratio_body, out_shape=arr(rows_dev, per_tile * side), compiler_params=params, name="coadd"
    )(*image_sum.parts(), weight_map)
    return (coadd, weight_map)


def solution(mesh):
    placed = (
        P("visit", "bulk", None, None, None),
        P("visit", "bulk", None, None, None),
        P("visit", "bulk", None, None, None),
        P("visit", "bulk", None, None, None),
        P("visit", "bulk", None, None),
        P("visit", "bulk", None),
        P("visit", "bulk", None, None),
        P(),
        P("visit", None),
    )
    return jax.shard_map(
        coadd_patches,
        mesh=mesh,
        in_specs=placed,
        out_specs=(P("bulk", "visit"), P("bulk", "visit")),
        check_vma=False,
    )
```

```python
import functools
import math

import jax
import jax.numpy as jnp
import numpy as np
from jax import lax
from jax.experimental import pallas as pl
from jax.experimental.pallas import tpu as pltpu
from jax.sharding import PartitionSpec as P


HALO = 64
BR = 2
BC = 8
CAP = 2
LANES = 128
VMEM_BYTES = 12 * 2**20
META = 8


F32 = jnp.float32
BF16 = jnp.bfloat16
VMEM = pl.BlockSpec(memory_space=pltpu.VMEM)
SMEM = pl.BlockSpec(memory_space=pltpu.SMEM)


def split(value):
    high = value.astype(BF16)
    low = (value - high.astype(F32)).astype(BF16)
    return high, low


def data(value, axis):
    high, low = split(value)
    return jnp.concatenate([high, low, high], axis)


def weights(value, axis):
    high, low = split(value)
    return jnp.concatenate([high, high, low], axis)


def table(value):
    value = np.asarray(value, np.float32)
    high = value.astype(jnp.bfloat16)
    return np.stack([high, (value - high.astype(np.float32)).astype(jnp.bfloat16)])


def fixed(ref, axis):
    return jnp.concatenate([ref[0], ref[0], ref[1]], axis)


def dot(a, b, dims=((1,), (0,))):
    return lax.dot_general(a, b, (dims, ((), ())), preferred_element_type=F32)


@functools.lru_cache
def make_tables(rows_dev, taps):
    length = rows_dev + taps - 1
    freqs = (length + 1) // 2
    k = np.arange(freqs)[:, None]

    def wave(first, second, period):
        return 2.0 * math.pi * ((first * second) % period) / period

    n = np.arange(rows_dev + 2 * HALO)[None, :] - 1
    theta = wave(k, n, length)
    used = n >= 0
    row_fwd = np.concatenate([np.cos(theta) * used, -np.sin(theta) * used], 0)
    theta = wave(k, np.arange(taps)[None, :], length)
    row_ker = np.concatenate([np.cos(theta), -np.sin(theta)], 0)
    period = 2 * taps
    n = np.arange(taps)[:, None]
    f = np.arange(taps)[None, :]
    col_fwd = []
    col_inv = []
    for odd in (0, 1):
        theta = wave(n, 2 * f + odd, period)
        c, s = np.cos(theta), np.sin(theta)
        col_fwd.append(np.block([[c, -s], [s, c]]))
        c, s = c.T, s.T
        sign = -1.0 if odd else 1.0
        col_inv.append(sign * np.block([[c, s], [-s, c]]))
    p = np.arange(rows_dev)[:, None] + taps - 1
    theta = wave(p, k.T, length)
    weight = np.where(k.T == 0, 1.0, 2.0) / (length * period)
    row_inv = np.concatenate([weight * np.cos(theta), -weight * np.sin(theta)], 1)
    return (
        table(row_fwd),
        table(row_ker),
        np.stack([table(t) for t in col_fwd]),
        np.stack([table(t) for t in col_inv]),
        table(row_inv),
    )


def partner(me, other):
    return jnp.bitwise_xor(me, other)


def places(ids, owner, slot):
    for q in range(slot.shape[2]):
        own = owner[0, 0, 0, q]
        rank = jnp.int32(0)
        for earlier in range(q):
            rank = rank + (owner[0, 0, 0, earlier] == own).astype(jnp.int32)
        yield q, partner(ids[0], own), own, rank, slot[0, 0, q]


def tile_at(ids, k, tiles):
    if tiles != 4:
        return jnp.int32(k)
    mine = jnp.int32(LINE[-1][k])
    for v in range(tiles - 1):
        mine = jnp.where(ids[1] == v, LINE[v][k], mine)
    return mine


def masked(extent, ivar, q):
    row_at = lax.broadcasted_iota(jnp.int32, ivar.shape, 0)
    col_at = lax.broadcasted_iota(jnp.int32, ivar.shape, 1)
    valid = (row_at < extent[0, 0, 0, q]) & (col_at < extent[0, 0, 1, q])
    return jnp.where(valid, ivar, 0.0)


def warp(plane, rows, cols):
    mid = dot(data(plane, 1), weights(cols, 1), ((1,), (1,)))
    return dot(weights(rows, 1), data(mid, 0))


def fetch(refs, buf, sems):
    copies = [
        [pltpu.make_async_copy(ref.at[0, 0, q], buf.at[i, q], sems.at[i, q]) for i, ref in enumerate(refs)]
        for q in range(buf.shape[1])
    ]
    for piece in copies:
        for copy in piece:
            copy.start()

    def get(q):
        for copy in copies[q]:
            copy.wait()
        return [buf[i, q] for i in range(len(refs))]

    return get


def run(copies):
    for copy in copies:
        copy.start()
    for copy in copies:
        copy.wait()


def warp_weight_body(ids, owner, slot, extent, ivar, rows, cols, *rest):
    side = ivar.shape[3]
    *outs, buf, buf_sems, send, sems = rest
    get = fetch((ivar, rows, cols), buf, buf_sems)
    for d in range(len(outs)):
        for rank in range(CAP):
            send[d, rank, side:, :] = jnp.full((META, side), -1.0, F32)
    for q, to, _, rank, at in places(ids, owner, slot):
        weight, row_map, col_map = get(q)
        send[to, rank, :side, :] = warp(masked(extent, weight, q), row_map, col_map)
        send[to, rank, side:, :] = jnp.full((META, side), at.astype(F32), F32)
    run([pltpu.make_async_copy(send.at[d], out, sems.at[d]) for d, out in enumerate(outs)])


def warp_flux_body(ids, owner, slot, extent, ivar, rows, cols, flux, out, buf, buf_sems):
    get = fetch((ivar, rows, cols, flux), buf, buf_sems)
    for q, _, own, rank, _ in places(ids, owner, slot):
        weight, row_map, col_map, value = get(q)
        out[own * CAP + rank] = warp(masked(extent, weight, q) * value, row_map, col_map)


def weight_body(ids, *rest):
    *rest, slot_out, acc, buf, sems = rest
    count = slot_out.shape[0] // CAP
    got, out = rest[:count], rest[count:]
    copies = [pltpu.make_async_copy(ref, buf.at[d], sems.at[d]) for d, ref in enumerate(got)]
    for copy in copies:
        copy.start()
    side = acc.shape[1]
    spare = acc.shape[0] - 1
    per_tile = out[0].shape[1] // side
    acc[...] = jnp.zeros(acc.shape, F32)
    for copy in copies:
        copy.wait()
    slots = []
    for d in range(count):
        for rank in range(CAP):
            at = jnp.max(buf[d, rank, side:, :]).astype(jnp.int32)
            slots.append(jnp.where(at < 0, spare, at))
    for n, at in enumerate(slots):
        d, rank = divmod(n, CAP)
        slot_out[partner(ids[0], d) * CAP + rank] = at
        acc[at] += buf[d, rank, :side, :]
    for k in range(len(out)):
        for c in range(per_tile):
            for r in range(BR):
                block = acc[r * BC + tile_at(ids, k, len(out)) * per_tile + c]
                out[k][r * side : (r + 1) * side, c * side : (c + 1) * side] = block


def image_body(ids, slot, got, *rest):
    *tiles, image, top, bottom, acc = rest
    side = acc.shape[1]
    per_tile = tiles[0].shape[1] // side
    acc[...] = jnp.zeros(acc.shape, F32)
    for n in range(slot.shape[0]):
        acc[slot[n]] += got[n]
    for k, tile in enumerate(tiles):
        for c in range(per_tile):
            to = tile_at(ids, k, len(tiles)) * per_tile + c
            for r in range(BR):
                rows = slice(r * side, (r + 1) * side)
                weight = tile[rows, c * side : (c + 1) * side]
                image[to, rows, :] = acc[r * BC + to] / jnp.maximum(weight, 1.0)
            top[to] = image[to, :HALO, :]
            bottom[to] = image[to, -HALO:, :]


def beside(stacked):
    n = stacked.shape[0] // 2
    return jnp.concatenate([stacked[:n], stacked[n:]], 1)


def spectrum_body(coeffs, basis, row_ker, col_fwd, out):
    kernel = coeffs[0, 0] * basis[0]
    for k in range(1, basis.shape[0]):
        kernel = kernel + coeffs[0, k] * basis[k]
    lines = data(beside(dot(fixed(row_ker, 1), data(kernel, 0))), 1)
    for odd in (0, 1):
        out[odd] = dot(lines, fixed(col_fwd.at[odd], 0))


def conv_body(first, tiles, ids, above, image, below, spec, row_fwd, col_fwd, col_inv, row_inv, *rest):
    *rest, lines = rest
    count = len(rest) // 2
    weight, out = rest[:count], rest[count:]
    taps = image.shape[2]
    per_tile = out[0].shape[1] // taps
    freqs = spec.shape[1]

    def column(c):
        return jnp.concatenate([above[c], image[c], below[c]], 0)

    lead = fixed(row_fwd, 1)
    last = fixed(row_inv, 1)
    for k in range(count):
        start = tile_at(ids, first + k, tiles) * per_tile
        parts = [column(start + c) for c in range(per_tile)]
        before = jnp.where(start > 0, column(jnp.maximum(start - 1, 0)), 0.0)
        after = jnp.where(start + per_tile < BC, column(jnp.minimum(start + per_tile, BC - 1)), 0.0)
        ext = jnp.concatenate([before[:, taps - HALO :], *parts, after[:, :HALO]], 1)
        lines[...] = dot(lead, data(ext, 0))
        one = [lines[:, c * taps : (c + 1) * taps] for c in range(per_tile + 1)]
        total = []
        for odd in (0, 1):
            mixed = [beside(a - b if odd else a + b) for a, b in zip(one, one[1:])]
            freq = dot(data(jnp.concatenate(mixed, 0), 1), fixed(col_fwd.at[odd], 0))
            kr = jnp.concatenate([spec[odd, :, :taps]] * per_tile, 0)
            ki = jnp.concatenate([spec[odd, :, taps:]] * per_tile, 0)
            zr, zi = freq[:, :taps], freq[:, taps:]
            prod = jnp.concatenate([zr * kr - zi * ki, zr * ki + zi * kr], 1)
            total.append(dot(data(prod, 1), fixed(col_inv.at[odd], 0)))
        wave = total[0] + total[1]
        parts = [wave[c * freqs : (c + 1) * freqs] for c in range(per_tile)]
        cols = [jnp.concatenate([p[:, :taps], p[:, taps:]], 0) for p in parts]
        out[k][...] = dot(last, data(jnp.concatenate(cols, 1), 0)) * weight[k][...]


LINE = ((3, 2, 1, 0), (2, 3, 0, 1), (1, 0, 3, 2), (0, 1, 2, 3))


class VisitSum:
    def __init__(self, count):
        self.count = count
        self.sent = []
        self.tiles = []

    def send(self, tile, *routes):
        self.sent += [lax.ppermute(tile, "visit", route) for route in routes]

    def push(self, *tiles):
        for tile in tiles:
            k = len(self.tiles)
            self.tiles.append(tile)
            if self.count != 4:
                continue
            if k == 0:
                self.send(tile, [(0, 1), (3, 2)])
                self.send(tile, [(1, 2), (2, 1)])
            elif k == 1:
                self.send(tile + self.sent[0], [(0, 2), (1, 3), (2, 0), (3, 1)])
            elif k == 2:
                self.send(tile, [(0, 1), (1, 0), (2, 3), (3, 2)])

    def parts(self):
        if self.count != 4:
            return [lax.psum_scatter(jnp.stack(self.tiles), "visit", scatter_dimension=0, tiled=False)]
        return [self.tiles[3], *self.sent[1:]]


def coadd_patches(piece_flux, piece_ivar, warp_rows, warp_cols, piece_owner, piece_slot, piece_extent, basis, coeffs):
    owners = lax.axis_size("bulk")
    visits = lax.axis_size("visit")
    pieces, side = piece_flux.shape[2:4]
    assert side == LANES and side == 2 * HALO and owners & (owners - 1) == 0
    rows_dev = BR * side
    per_tile = BC // visits
    cap = owners * CAP
    row_fwd, row_ker, col_fwd, col_inv, row_inv = [jnp.asarray(t) for t in make_tables(rows_dev, side)]
    freqs = row_fwd.shape[1] // 2
    ids = jnp.stack([lax.axis_index("bulk"), lax.axis_index("visit")]).astype(jnp.int32)
    facts = (ids, piece_owner.transpose(0, 1, 3, 2), piece_slot, piece_extent.transpose(0, 1, 3, 2))

    params = pltpu.CompilerParams(vmem_limit_bytes=VMEM_BYTES)

    def arr(*shape):
        return jax.ShapeDtypeStruct(shape, F32)

    hbm = pl.BlockSpec(memory_space=pltpu.HBM)

    def piece_buffers(count):
        return [pltpu.VMEM((count, pieces, side, side), F32), pltpu.SemaphoreType.DMA((count, pieces))]

    def exchange(sent):
        got = [sent[0]]
        for d in range(1, owners):
            got.append(lax.ppermute(sent[d], "bulk", [(i, i ^ d) for i in range(owners)]))
        return got

    sent_weight = pl.pallas_call(
        warp_weight_body,
        out_shape=[arr(CAP, side + META, side)] * owners,
        in_specs=[SMEM] * 4 + [hbm] * 3,
        out_specs=[hbm] * owners,
        scratch_shapes=piece_buffers(3)
        + [pltpu.VMEM((owners, CAP, side + META, side), F32), pltpu.SemaphoreType.DMA((owners,))],
        compiler_params=params,
        name="warp_weight",
    )(*facts, piece_ivar, warp_rows, warp_cols)
    got_weight = exchange(sent_weight)
    sent_flux = pl.pallas_call(
        warp_flux_body,
        out_shape=arr(cap, side, side),
        in_specs=[SMEM] * 4 + [hbm] * 4,
        out_specs=VMEM,
        scratch_shapes=piece_buffers(4),
        compiler_params=params,
        name="warp_flux",
    )(*facts, piece_ivar, warp_rows, warp_cols, piece_flux)
    got_flux = lax.all_to_all(sent_flux, "bulk", split_axis=0, concat_axis=0, tiled=True)
    spec = pl.pallas_call(
        spectrum_body,
        out_shape=arr(2, freqs, 2 * side),
        in_specs=[SMEM] + [VMEM] * 3,
        out_specs=VMEM,
        compiler_params=params,
        name="spectrum",
    )(coeffs, basis, row_ker, col_fwd)
    tile = arr(rows_dev, per_tile * side)
    *ivar, slots = pl.pallas_call(
        weight_body,
        out_shape=[tile] * visits + [jax.ShapeDtypeStruct((cap,), jnp.int32)],
        in_specs=[SMEM] + [hbm] * owners,
        out_specs=[VMEM] * visits + [SMEM],
        scratch_shapes=[
            pltpu.VMEM((BR * BC + 1, side, side), F32),
            pltpu.VMEM((owners, CAP, side + META, side), F32),
            pltpu.SemaphoreType.DMA((owners,)),
        ],
        compiler_params=params,
        name="weights",
    )(ids, *got_weight)
    weight_sum = VisitSum(visits)
    weight_sum.push(*ivar)
    image, top, bottom = pl.pallas_call(
        image_body,
        out_shape=[arr(BC, rows_dev, side)] + [arr(BC, HALO, side)] * 2,
        in_specs=[SMEM] * 2 + [VMEM] * (1 + visits),
        out_specs=[VMEM] * 3,
        scratch_shapes=[pltpu.VMEM((BR * BC + 1, side, side), F32)],
        compiler_params=params,
        name="image",
    )(ids, slots, got_flux, *ivar)
    ends = owners - 1
    above = lax.ppermute(bottom, "bulk", [(i, i + 1) for i in range(ends)])
    below = lax.ppermute(top, "bulk", [(i + 1, i) for i in range(ends)])
    weight_map = functools.reduce(jnp.add, weight_sum.parts())

    def convolve(first, count):
        return pl.pallas_call(
            functools.partial(conv_body, first, visits),
            out_shape=[tile] * count,
            in_specs=[SMEM] + [VMEM] * (8 + count),
            out_specs=[VMEM] * count,
            scratch_shapes=[pltpu.VMEM((2 * freqs, (per_tile + 1) * side), F32)],
            compiler_params=params,
        )(ids, above, image, below, spec, row_fwd, col_fwd, col_inv, row_inv, *ivar[first : first + count])

    image_sum = VisitSum(visits)
    image_sum.push(*convolve(0, 1))
    image_sum.push(*convolve(1, visits - 2))
    image_sum.push(*convolve(visits - 1, 1))
    numerator = functools.reduce(jnp.add, image_sum.parts())
    return (numerator / jnp.maximum(weight_map, 1.0), weight_map)


def solution(mesh):
    placed = (
        P("visit", "bulk", None, None, None),
        P("visit", "bulk", None, None, None),
        P("visit", "bulk", None, None, None),
        P("visit", "bulk", None, None, None),
        P("visit", "bulk", None, None),
        P("visit", "bulk", None),
        P("visit", "bulk", None, None),
        P(),
        P("visit", None),
    )
    return jax.shard_map(
        coadd_patches,
        mesh=mesh,
        in_specs=placed,
        out_specs=(P("bulk", "visit"), P("bulk", "visit")),
        check_vma=False,
    )
```

```python
import functools
import math

import jax
import jax.numpy as jnp
import numpy as np
from jax import lax
from jax.experimental import pallas as pl
from jax.experimental.pallas import tpu as pltpu
from jax.sharding import PartitionSpec as P


HALO = 64
BR = 2
BC = 8
CAP = 2
LANES = 128
VMEM_BYTES = 12 * 2**20
META = 8


F32 = jnp.float32
BF16 = jnp.bfloat16
VMEM = pl.BlockSpec(memory_space=pltpu.VMEM)
SMEM = pl.BlockSpec(memory_space=pltpu.SMEM)


def split(value):
    high = value.astype(BF16)
    low = (value - high.astype(F32)).astype(BF16)
    return high, low


def data(value, axis):
    high, low = split(value)
    return jnp.concatenate([high, low, high], axis)


def weights(value, axis):
    high, low = split(value)
    return jnp.concatenate([high, high, low], axis)


def table(value):
    value = np.asarray(value, np.float32)
    high = value.astype(jnp.bfloat16)
    return np.stack([high, (value - high.astype(np.float32)).astype(jnp.bfloat16)])


def fixed(ref, axis):
    return jnp.concatenate([ref[0], ref[0], ref[1]], axis)


def dot(a, b, dims=((1,), (0,))):
    return lax.dot_general(a, b, (dims, ((), ())), preferred_element_type=F32)


@functools.lru_cache
def make_tables(rows_dev, taps):
    length = rows_dev + taps - 1
    freqs = (length + 1) // 2
    k = np.arange(freqs)[:, None]

    def wave(first, second, period):
        return 2.0 * math.pi * ((first * second) % period) / period

    n = np.arange(rows_dev + 2 * HALO)[None, :] - 1
    theta = wave(k, n, length)
    used = n >= 0
    row_fwd = np.concatenate([np.cos(theta) * used, -np.sin(theta) * used], 0)
    theta = wave(k, np.arange(taps)[None, :], length)
    row_ker = np.concatenate([np.cos(theta), -np.sin(theta)], 0)
    period = 2 * taps
    n = np.arange(taps)[:, None]
    f = np.arange(taps)[None, :]
    col_fwd = []
    col_inv = []
    for odd in (0, 1):
        theta = wave(n, 2 * f + odd, period)
        c, s = np.cos(theta), np.sin(theta)
        col_fwd.append(np.block([[c, -s], [s, c]]))
        c, s = c.T, s.T
        sign = -1.0 if odd else 1.0
        col_inv.append(sign * np.block([[c, s], [-s, c]]))
    p = np.arange(rows_dev)[:, None] + taps - 1
    theta = wave(p, k.T, length)
    weight = np.where(k.T == 0, 1.0, 2.0) / (length * period)
    row_inv = np.concatenate([weight * np.cos(theta), -weight * np.sin(theta)], 1)
    return (
        table(row_fwd),
        table(row_ker),
        np.stack([table(t) for t in col_fwd]),
        np.stack([table(t) for t in col_inv]),
        table(row_inv),
    )


def partner(me, other):
    return jnp.bitwise_xor(me, other)


def places(ids, owner, slot):
    for q in range(slot.shape[2]):
        own = owner[0, 0, 0, q]
        rank = jnp.int32(0)
        for earlier in range(q):
            rank = rank + (owner[0, 0, 0, earlier] == own).astype(jnp.int32)
        yield q, partner(ids[0], own), own, rank, slot[0, 0, q]


def tile_at(ids, k, tiles):
    if tiles != 4:
        return jnp.int32(k)
    mine = jnp.int32(LINE[-1][k])
    for v in range(tiles - 1):
        mine = jnp.where(ids[1] == v, LINE[v][k], mine)
    return mine


def masked(extent, ivar, q):
    row_at = lax.broadcasted_iota(jnp.int32, ivar.shape, 0)
    col_at = lax.broadcasted_iota(jnp.int32, ivar.shape, 1)
    valid = (row_at < extent[0, 0, 0, q]) & (col_at < extent[0, 0, 1, q])
    return jnp.where(valid, ivar, 0.0)


def warp(plane, rows, cols):
    mid = dot(data(plane, 1), weights(cols, 1), ((1,), (1,)))
    return dot(weights(rows, 1), data(mid, 0))


def run(copies):
    for copy in copies:
        copy.start()
    for copy in copies:
        copy.wait()


def warp_weight_body(ids, owner, slot, extent, ivar_far, rows_far, cols_far, flux_far, *rest):
    *outs, ivar, rows, cols, flux, send, sems = rest
    side = ivar.shape[3]
    later = pltpu.make_async_copy(flux_far, flux, sems.at[3])
    far = (ivar_far, rows_far, cols_far)
    copies = [pltpu.make_async_copy(a, b, sems.at[n]) for n, (a, b) in enumerate(zip(far, (ivar, rows, cols)))]
    for copy in [*copies, later]:
        copy.start()
    for d in range(len(outs)):
        for rank in range(CAP):
            send[d, rank, side:, :] = jnp.full((META, side), -1.0, F32)
    for copy in copies:
        copy.wait()
    for q, to, _, rank, at in places(ids, owner, slot):
        send[to, rank, :side, :] = warp(masked(extent, ivar[0, 0, q], q), rows[0, 0, q], cols[0, 0, q])
        send[to, rank, side:, :] = jnp.full((META, side), at.astype(F32), F32)
    for d, out in enumerate(outs):
        out[...] = send[d]
    later.wait()


def warp_flux_body(ids, owner, slot, extent, ivar, rows, cols, flux, out):
    for q, _, own, rank, _ in places(ids, owner, slot):
        plane = masked(extent, ivar[0, 0, q], q) * flux[0, 0, q]
        out[own * CAP + rank] = warp(plane, rows[0, 0, q], cols[0, 0, q])


def weight_body(ids, own, *rest):
    *rest, slot_out, acc, buf, sems = rest
    count = slot_out.shape[0] // CAP
    far, out = rest[: count - 1], rest[count - 1 :]
    run([pltpu.make_async_copy(ref, buf.at[d], sems.at[d]) for d, ref in enumerate(far)])
    got = [own] + [buf.at[d] for d in range(count - 1)]
    side = acc.shape[1]
    spare = acc.shape[0] - 1
    per_tile = out[0].shape[1] // side
    acc[...] = jnp.zeros(acc.shape, F32)
    slots = []
    for d in range(count):
        for rank in range(CAP):
            at = jnp.max(got[d][rank, side:, :]).astype(jnp.int32)
            slots.append(jnp.where(at < 0, spare, at))
    for n, at in enumerate(slots):
        d, rank = divmod(n, CAP)
        slot_out[partner(ids[0], d) * CAP + rank] = at
        acc[at] += got[d][rank, :side, :]
    for k in range(len(out)):
        for c in range(per_tile):
            for r in range(BR):
                block = acc[r * BC + tile_at(ids, k, len(out)) * per_tile + c]
                out[k][r * side : (r + 1) * side, c * side : (c + 1) * side] = block


def image_body(ids, slot, got, *rest):
    *tiles, image, top, bottom, acc = rest
    side = acc.shape[1]
    per_tile = tiles[0].shape[1] // side
    acc[...] = jnp.zeros(acc.shape, F32)
    for n in range(slot.shape[0]):
        acc[slot[n]] += got[n]
    for k, tile in enumerate(tiles):
        for c in range(per_tile):
            to = tile_at(ids, k, len(tiles)) * per_tile + c
            for r in range(BR):
                rows = slice(r * side, (r + 1) * side)
                weight = tile[rows, c * side : (c + 1) * side]
                image[to, rows, :] = acc[r * BC + to] / jnp.maximum(weight, 1.0)
            top[to] = image[to, :HALO, :]
            bottom[to] = image[to, -HALO:, :]


def beside(stacked):
    n = stacked.shape[0] // 2
    return jnp.concatenate([stacked[:n], stacked[n:]], 1)


def spectrum_body(coeffs, basis, row_ker, col_fwd, out):
    kernel = coeffs[0, 0] * basis[0]
    for k in range(1, basis.shape[0]):
        kernel = kernel + coeffs[0, k] * basis[k]
    lines = data(beside(dot(fixed(row_ker, 1), data(kernel, 0))), 1)
    for odd in (0, 1):
        out[odd] = dot(lines, fixed(col_fwd.at[odd], 0))


def conv_body(first, tiles, ids, above, image, below, spec, row_fwd, col_fwd, col_inv, row_inv, *rest):
    *rest, lines = rest
    count = len(rest) // 2
    weight, out = rest[:count], rest[count:]
    taps = image.shape[2]
    per_tile = out[0].shape[1] // taps
    freqs = spec.shape[1]

    def column(c):
        return jnp.concatenate([above[c], image[c], below[c]], 0)

    lead = fixed(row_fwd, 1)
    last = fixed(row_inv, 1)
    for k in range(count):
        start = tile_at(ids, first + k, tiles) * per_tile
        parts = [column(start + c) for c in range(per_tile)]
        before = jnp.where(start > 0, column(jnp.maximum(start - 1, 0)), 0.0)
        after = jnp.where(start + per_tile < BC, column(jnp.minimum(start + per_tile, BC - 1)), 0.0)
        ext = jnp.concatenate([before[:, taps - HALO :], *parts, after[:, :HALO]], 1)
        lines[...] = dot(lead, data(ext, 0))
        one = [lines[:, c * taps : (c + 1) * taps] for c in range(per_tile + 1)]
        total = []
        for odd in (0, 1):
            mixed = [beside(a - b if odd else a + b) for a, b in zip(one, one[1:])]
            freq = dot(data(jnp.concatenate(mixed, 0), 1), fixed(col_fwd.at[odd], 0))
            kr = jnp.concatenate([spec[odd, :, :taps]] * per_tile, 0)
            ki = jnp.concatenate([spec[odd, :, taps:]] * per_tile, 0)
            zr, zi = freq[:, :taps], freq[:, taps:]
            prod = jnp.concatenate([zr * kr - zi * ki, zr * ki + zi * kr], 1)
            total.append(dot(data(prod, 1), fixed(col_inv.at[odd], 0)))
        wave = total[0] + total[1]
        parts = [wave[c * freqs : (c + 1) * freqs] for c in range(per_tile)]
        cols = [jnp.concatenate([p[:, :taps], p[:, taps:]], 0) for p in parts]
        out[k][...] = dot(last, data(jnp.concatenate(cols, 1), 0)) * weight[k][...]


LINE = ((3, 2, 1, 0), (2, 3, 0, 1), (1, 0, 3, 2), (0, 1, 2, 3))


class VisitSum:
    def __init__(self, count):
        self.count = count
        self.sent = []
        self.tiles = []

    def send(self, tile, *routes):
        self.sent += [lax.ppermute(tile, "visit", route) for route in routes]

    def push(self, *tiles):
        for tile in tiles:
            k = len(self.tiles)
            self.tiles.append(tile)
            if self.count != 4:
                continue
            if k == 0:
                self.send(tile, [(0, 1), (3, 2)])
                self.send(tile, [(1, 2), (2, 1)])
            elif k == 1:
                self.send(tile + self.sent[0], [(0, 2), (1, 3), (2, 0), (3, 1)])
            elif k == 2:
                self.send(tile, [(0, 1), (1, 0), (2, 3), (3, 2)])

    def parts(self):
        if self.count != 4:
            return [lax.psum_scatter(jnp.stack(self.tiles), "visit", scatter_dimension=0, tiled=False)]
        return [self.tiles[3], *self.sent[1:]]


def coadd_patches(piece_flux, piece_ivar, warp_rows, warp_cols, piece_owner, piece_slot, piece_extent, basis, coeffs):
    owners = lax.axis_size("bulk")
    visits = lax.axis_size("visit")
    _, side = piece_flux.shape[2:4]
    assert side == LANES and side == 2 * HALO and owners & (owners - 1) == 0
    rows_dev = BR * side
    per_tile = BC // visits
    cap = owners * CAP
    row_fwd, row_ker, col_fwd, col_inv, row_inv = [jnp.asarray(t) for t in make_tables(rows_dev, side)]
    freqs = row_fwd.shape[1] // 2
    ids = jnp.stack([lax.axis_index("bulk"), lax.axis_index("visit")]).astype(jnp.int32)
    facts = (ids, piece_owner.transpose(0, 1, 3, 2), piece_slot, piece_extent.transpose(0, 1, 3, 2))

    params = pltpu.CompilerParams(vmem_limit_bytes=VMEM_BYTES)

    def arr(*shape):
        return jax.ShapeDtypeStruct(shape, F32)

    hbm = pl.BlockSpec(memory_space=pltpu.HBM)

    def in_hbm(*arrays):
        return [pltpu.with_memory_space_constraint(a, pltpu.HBM) for a in arrays]

    def exchange(sent):
        got = [sent[0]]
        for d in range(1, owners):
            got.append(lax.ppermute(sent[d], "bulk", [(i, i ^ d) for i in range(owners)]))
        return got

    *sent_weight, ivar_near, rows_near, cols_near, flux_near = pl.pallas_call(
        warp_weight_body,
        out_shape=[arr(CAP, side + META, side)] * owners + [arr(*piece_flux.shape)] * 4,
        in_specs=[SMEM] * 4 + [hbm] * 4,
        out_specs=[VMEM] * (owners + 4),
        scratch_shapes=[pltpu.VMEM((owners, CAP, side + META, side), F32), pltpu.SemaphoreType.DMA((4,))],
        compiler_params=params,
        name="warp_weight",
    )(*facts, *in_hbm(piece_ivar, warp_rows, warp_cols, piece_flux))
    got_weight = exchange(sent_weight)
    sent_flux = pl.pallas_call(
        warp_flux_body,
        out_shape=arr(cap, side, side),
        in_specs=[SMEM] * 4 + [VMEM] * 4,
        out_specs=VMEM,
        compiler_params=params,
        name="warp_flux",
    )(*facts, ivar_near, rows_near, cols_near, flux_near)
    got_flux = lax.all_to_all(sent_flux, "bulk", split_axis=0, concat_axis=0, tiled=True)
    spec = pl.pallas_call(
        spectrum_body,
        out_shape=arr(2, freqs, 2 * side),
        in_specs=[SMEM] + [VMEM] * 3,
        out_specs=VMEM,
        compiler_params=params,
        name="spectrum",
    )(coeffs, basis, row_ker, col_fwd)
    tile = arr(rows_dev, per_tile * side)
    *ivar, slots = pl.pallas_call(
        weight_body,
        out_shape=[tile] * visits + [jax.ShapeDtypeStruct((cap,), jnp.int32)],
        in_specs=[SMEM, VMEM] + [hbm] * (owners - 1),
        out_specs=[VMEM] * visits + [SMEM],
        scratch_shapes=[
            pltpu.VMEM((BR * BC + 1, side, side), F32),
            pltpu.VMEM((owners - 1, CAP, side + META, side), F32),
            pltpu.SemaphoreType.DMA((owners - 1,)),
        ],
        compiler_params=params,
        name="weights",
    )(ids, got_weight[0], *in_hbm(*got_weight[1:]))
    weight_sum = VisitSum(visits)
    weight_sum.push(*ivar)
    image, top, bottom = pl.pallas_call(
        image_body,
        out_shape=[arr(BC, rows_dev, side)] + [arr(BC, HALO, side)] * 2,
        in_specs=[SMEM] * 2 + [VMEM] * (1 + visits),
        out_specs=[VMEM] * 3,
        scratch_shapes=[pltpu.VMEM((BR * BC + 1, side, side), F32)],
        compiler_params=params,
        name="image",
    )(ids, slots, got_flux, *ivar)
    ends = owners - 1
    above = lax.ppermute(bottom, "bulk", [(i, i + 1) for i in range(ends)])
    below = lax.ppermute(top, "bulk", [(i + 1, i) for i in range(ends)])
    weight_map = lax.optimization_barrier(functools.reduce(jnp.add, weight_sum.parts()))

    def convolve(first, count):
        return pl.pallas_call(
            functools.partial(conv_body, first, visits),
            out_shape=[tile] * count,
            in_specs=[SMEM] + [VMEM] * (8 + count),
            out_specs=[VMEM] * count,
            scratch_shapes=[pltpu.VMEM((2 * freqs, (per_tile + 1) * side), F32)],
            compiler_params=params,
        )(ids, above, image, below, spec, row_fwd, col_fwd, col_inv, row_inv, *ivar[first : first + count])

    image_sum = VisitSum(visits)
    image_sum.push(*convolve(0, 1))
    image_sum.push(*convolve(1, visits - 2))
    image_sum.push(*convolve(visits - 1, 1))
    numerator = functools.reduce(jnp.add, image_sum.parts())
    return (numerator / jnp.maximum(weight_map, 1.0), weight_map)


def solution(mesh):
    placed = (
        P("visit", "bulk", None, None, None),
        P("visit", "bulk", None, None, None),
        P("visit", "bulk", None, None, None),
        P("visit", "bulk", None, None, None),
        P("visit", "bulk", None, None),
        P("visit", "bulk", None),
        P("visit", "bulk", None, None),
        P(),
        P("visit", None),
    )
    return jax.shard_map(
        coadd_patches,
        mesh=mesh,
        in_specs=placed,
        out_specs=(P("bulk", "visit"), P("bulk", "visit")),
        check_vma=False,
    )
```

```python
import functools
import math

import jax
import jax.numpy as jnp
import numpy as np
from jax import lax
from jax.experimental import pallas as pl
from jax.experimental.pallas import tpu as pltpu
from jax.sharding import PartitionSpec as P


HALO = 64
BR = 2
BC = 8
CAP = 2
LANES = 128
VMEM_BYTES = 12 * 2**20
META = 8


F32 = jnp.float32
BF16 = jnp.bfloat16
VMEM = pl.BlockSpec(memory_space=pltpu.VMEM)
SMEM = pl.BlockSpec(memory_space=pltpu.SMEM)


def split(value):
    high = value.astype(BF16)
    low = (value - high.astype(F32)).astype(BF16)
    return high, low


def data(value, axis):
    high, low = split(value)
    return jnp.concatenate([high, low, high], axis)


def weights(value, axis):
    high, low = split(value)
    return jnp.concatenate([high, high, low], axis)


def table(value):
    value = np.asarray(value, np.float32)
    high = value.astype(jnp.bfloat16)
    return np.stack([high, (value - high.astype(np.float32)).astype(jnp.bfloat16)])


def fixed(ref, axis):
    return jnp.concatenate([ref[0], ref[0], ref[1]], axis)


def dot(a, b, dims=((1,), (0,))):
    return lax.dot_general(a, b, (dims, ((), ())), preferred_element_type=F32)


@functools.lru_cache
def make_tables(rows_dev, taps):
    length = rows_dev + taps - 1
    freqs = (length + 1) // 2
    k = np.arange(freqs)[:, None]

    def wave(first, second, period):
        return 2.0 * math.pi * ((first * second) % period) / period

    n = np.arange(rows_dev + 2 * HALO)[None, :] - 1
    theta = wave(k, n, length)
    used = n >= 0
    row_fwd = np.concatenate([np.cos(theta) * used, -np.sin(theta) * used], 0)
    theta = wave(k, np.arange(taps)[None, :], length)
    row_ker = np.concatenate([np.cos(theta), -np.sin(theta)], 0)
    period = 2 * taps
    n = np.arange(taps)[:, None]
    f = np.arange(taps)[None, :]
    col_fwd = []
    col_inv = []
    for odd in (0, 1):
        theta = wave(n, 2 * f + odd, period)
        c, s = np.cos(theta), np.sin(theta)
        col_fwd.append(np.block([[c, -s], [s, c]]))
        c, s = c.T, s.T
        sign = -1.0 if odd else 1.0
        col_inv.append(sign * np.block([[c, s], [-s, c]]))
    p = np.arange(rows_dev)[:, None] + taps - 1
    theta = wave(p, k.T, length)
    weight = np.where(k.T == 0, 1.0, 2.0) / (length * period)
    row_inv = np.concatenate([weight * np.cos(theta), -weight * np.sin(theta)], 1)
    return (
        table(row_fwd),
        table(row_ker),
        np.stack([table(t) for t in col_fwd]),
        np.stack([table(t) for t in col_inv]),
        table(row_inv),
    )


def partner(me, other):
    return jnp.bitwise_xor(me, other)


def places(ids, owner, slot):
    for q in range(slot.shape[2]):
        own = owner[0, 0, 0, q]
        rank = jnp.int32(0)
        for earlier in range(q):
            rank = rank + (owner[0, 0, 0, earlier] == own).astype(jnp.int32)
        yield q, partner(ids[0], own), own, rank, slot[0, 0, q]


def tile_at(ids, k, tiles):
    return jnp.bitwise_xor(ids[1], tiles - 1 - k)


def masked(extent, ivar, q):
    row_at = lax.broadcasted_iota(jnp.int32, ivar.shape, 0)
    col_at = lax.broadcasted_iota(jnp.int32, ivar.shape, 1)
    valid = (row_at < extent[0, 0, 0, q]) & (col_at < extent[0, 0, 1, q])
    return jnp.where(valid, ivar, 0.0)


def warp(plane, rows, cols):
    mid = dot(data(plane, 1), weights(cols, 1), ((1,), (1,)))
    return dot(weights(rows, 1), data(mid, 0))


def run(copies):
    for copy in copies:
        copy.start()
    for copy in copies:
        copy.wait()


def warp_weight_body(ids, owner, slot, extent, ivar_far, rows_far, cols_far, flux_far, *rest):
    *outs, ivar, rows, cols, flux, send, sems = rest
    side = ivar.shape[3]
    later = pltpu.make_async_copy(flux_far, flux, sems.at[3])
    far = (ivar_far, rows_far, cols_far)
    copies = [pltpu.make_async_copy(a, b, sems.at[n]) for n, (a, b) in enumerate(zip(far, (ivar, rows, cols)))]
    for copy in [*copies, later]:
        copy.start()
    for d in range(len(outs)):
        for rank in range(CAP):
            send[d, rank, side:, :] = jnp.full((META, side), -1.0, F32)
    for copy in copies:
        copy.wait()
    for q, to, _, rank, at in places(ids, owner, slot):
        send[to, rank, :side, :] = warp(masked(extent, ivar[0, 0, q], q), rows[0, 0, q], cols[0, 0, q])
        send[to, rank, side:, :] = jnp.full((META, side), at.astype(F32), F32)
    for d, out in enumerate(outs):
        out[...] = send[d]
    later.wait()


def warp_flux_body(ids, owner, slot, extent, ivar, rows, cols, flux, out):
    for q, _, own, rank, _ in places(ids, owner, slot):
        plane = masked(extent, ivar[0, 0, q], q) * flux[0, 0, q]
        out[own * CAP + rank] = warp(plane, rows[0, 0, q], cols[0, 0, q])


def weight_body(ids, own, *rest):
    *rest, slot_out, acc, buf, sems = rest
    count = slot_out.shape[0] // CAP
    far, out = rest[: count - 1], rest[count - 1 :]
    run([pltpu.make_async_copy(ref, buf.at[d], sems.at[d]) for d, ref in enumerate(far)])
    got = [own] + [buf.at[d] for d in range(count - 1)]
    side = acc.shape[1]
    spare = acc.shape[0] - 1
    per_tile = out[0].shape[1] // side
    acc[...] = jnp.zeros(acc.shape, F32)
    slots = []
    for d in range(count):
        for rank in range(CAP):
            at = jnp.max(got[d][rank, side:, :]).astype(jnp.int32)
            slots.append(jnp.where(at < 0, spare, at))
    for n, at in enumerate(slots):
        d, rank = divmod(n, CAP)
        slot_out[partner(ids[0], d) * CAP + rank] = at
        acc[at] += got[d][rank, :side, :]
    for k in range(len(out)):
        for c in range(per_tile):
            for r in range(BR):
                block = acc[r * BC + tile_at(ids, k, len(out)) * per_tile + c]
                out[k][r * side : (r + 1) * side, c * side : (c + 1) * side] = block


def image_body(ids, slot, got, *rest):
    *tiles, image, near, far, acc = rest
    odd_strip = ids[0] % 2 == 1
    side = acc.shape[1]
    per_tile = tiles[0].shape[1] // side
    acc[...] = jnp.zeros(acc.shape, F32)
    for n in range(slot.shape[0]):
        acc[slot[n]] += got[n]
    for k, tile in enumerate(tiles):
        for c in range(per_tile):
            to = tile_at(ids, k, len(tiles)) * per_tile + c
            for r in range(BR):
                rows = slice(r * side, (r + 1) * side)
                weight = tile[rows, c * side : (c + 1) * side]
                image[to, rows, :] = acc[r * BC + to] / jnp.maximum(weight, 1.0)
            top, bottom = image[to, :HALO, :], image[to, -HALO:, :]
            near[to] = jnp.where(odd_strip, top, bottom)
            far[to] = jnp.where(odd_strip, bottom, top)


def beside(stacked):
    n = stacked.shape[0] // 2
    return jnp.concatenate([stacked[:n], stacked[n:]], 1)


def spectrum_body(coeffs, basis, row_ker, col_fwd, out):
    kernel = coeffs[0, 0] * basis[0]
    for k in range(1, basis.shape[0]):
        kernel = kernel + coeffs[0, k] * basis[k]
    lines = data(beside(dot(fixed(row_ker, 1), data(kernel, 0))), 1)
    for odd in (0, 1):
        out[odd] = dot(lines, fixed(col_fwd.at[odd], 0))


def conv_body(first, tiles, ids, near, image, far, spec, row_fwd, col_fwd, col_inv, row_inv, *rest):
    *rest, lines = rest
    count = len(rest) // 2
    weight, out = rest[:count], rest[count:]
    taps = image.shape[2]
    per_tile = out[0].shape[1] // taps
    freqs = spec.shape[1]
    odd_strip = ids[0] % 2 == 1

    def column(c):
        above = jnp.where(odd_strip, near[c], far[c])
        below = jnp.where(odd_strip, far[c], near[c])
        return jnp.concatenate([above, image[c], below], 0)

    lead = fixed(row_fwd, 1)
    last = fixed(row_inv, 1)
    for k in range(count):
        start = tile_at(ids, first + k, tiles) * per_tile
        parts = [column(start + c) for c in range(per_tile)]
        before = jnp.where(start > 0, column(jnp.maximum(start - 1, 0)), 0.0)
        after = jnp.where(start + per_tile < BC, column(jnp.minimum(start + per_tile, BC - 1)), 0.0)
        ext = jnp.concatenate([before[:, taps - HALO :], *parts, after[:, :HALO]], 1)
        lines[...] = dot(lead, data(ext, 0))
        one = [lines[:, c * taps : (c + 1) * taps] for c in range(per_tile + 1)]
        total = []
        for odd in (0, 1):
            mixed = [beside(a - b if odd else a + b) for a, b in zip(one, one[1:])]
            freq = dot(data(jnp.concatenate(mixed, 0), 1), fixed(col_fwd.at[odd], 0))
            kr = jnp.concatenate([spec[odd, :, :taps]] * per_tile, 0)
            ki = jnp.concatenate([spec[odd, :, taps:]] * per_tile, 0)
            zr, zi = freq[:, :taps], freq[:, taps:]
            prod = jnp.concatenate([zr * kr - zi * ki, zr * ki + zi * kr], 1)
            total.append(dot(data(prod, 1), fixed(col_inv.at[odd], 0)))
        wave = total[0] + total[1]
        parts = [wave[c * freqs : (c + 1) * freqs] for c in range(per_tile)]
        cols = [jnp.concatenate([p[:, :taps], p[:, taps:]], 0) for p in parts]
        out[k][...] = dot(last, data(jnp.concatenate(cols, 1), 0)) * weight[k][...]


def send_tile(tile, k):
    visits = lax.axis_size("visit")
    return lax.ppermute(tile, "visit", [(v, v ^ (visits - 1 - k)) for v in range(visits)])


def coadd_patches(piece_flux, piece_ivar, warp_rows, warp_cols, piece_owner, piece_slot, piece_extent, basis, coeffs):
    owners = lax.axis_size("bulk")
    visits = lax.axis_size("visit")
    _, side = piece_flux.shape[2:4]
    assert side == LANES and side == 2 * HALO and owners & (owners - 1) == 0
    rows_dev = BR * side
    per_tile = BC // visits
    cap = owners * CAP
    row_fwd, row_ker, col_fwd, col_inv, row_inv = [jnp.asarray(t) for t in make_tables(rows_dev, side)]
    freqs = row_fwd.shape[1] // 2
    ids = jnp.stack([lax.axis_index("bulk"), lax.axis_index("visit")]).astype(jnp.int32)
    facts = (ids, piece_owner.transpose(0, 1, 3, 2), piece_slot, piece_extent.transpose(0, 1, 3, 2))

    params = pltpu.CompilerParams(vmem_limit_bytes=VMEM_BYTES)

    def arr(*shape):
        return jax.ShapeDtypeStruct(shape, F32)

    hbm = pl.BlockSpec(memory_space=pltpu.HBM)

    def in_hbm(*arrays):
        return [pltpu.with_memory_space_constraint(a, pltpu.HBM) for a in arrays]

    def exchange(sent):
        got = [sent[0]]
        for d in range(1, owners):
            got.append(lax.ppermute(sent[d], "bulk", [(i, i ^ d) for i in range(owners)]))
        return got

    *sent_weight, ivar_near, rows_near, cols_near, flux_near = pl.pallas_call(
        warp_weight_body,
        out_shape=[arr(CAP, side + META, side)] * owners + [arr(*piece_flux.shape)] * 4,
        in_specs=[SMEM] * 4 + [hbm] * 4,
        out_specs=[VMEM] * (owners + 4),
        scratch_shapes=[pltpu.VMEM((owners, CAP, side + META, side), F32), pltpu.SemaphoreType.DMA((4,))],
        compiler_params=params,
        name="warp_weight",
    )(*facts, *in_hbm(piece_ivar, warp_rows, warp_cols, piece_flux))
    got_weight = exchange(sent_weight)
    sent_flux = pl.pallas_call(
        warp_flux_body,
        out_shape=arr(cap, side, side),
        in_specs=[SMEM] * 4 + [VMEM] * 4,
        out_specs=VMEM,
        compiler_params=params,
        name="warp_flux",
    )(*facts, ivar_near, rows_near, cols_near, flux_near)
    got_flux = lax.all_to_all(sent_flux, "bulk", split_axis=0, concat_axis=0, tiled=True)
    spec = pl.pallas_call(
        spectrum_body,
        out_shape=arr(2, freqs, 2 * side),
        in_specs=[SMEM] + [VMEM] * 3,
        out_specs=VMEM,
        compiler_params=params,
        name="spectrum",
    )(coeffs, basis, row_ker, col_fwd)
    tile = arr(rows_dev, per_tile * side)
    *ivar, slots = pl.pallas_call(
        weight_body,
        out_shape=[tile] * visits + [jax.ShapeDtypeStruct((cap,), jnp.int32)],
        in_specs=[SMEM, VMEM] + [hbm] * (owners - 1),
        out_specs=[VMEM] * visits + [SMEM],
        scratch_shapes=[
            pltpu.VMEM((BR * BC + 1, side, side), F32),
            pltpu.VMEM((owners - 1, CAP, side + META, side), F32),
            pltpu.SemaphoreType.DMA((owners - 1,)),
        ],
        compiler_params=params,
        name="weights",
    )(ids, got_weight[0], *in_hbm(*got_weight[1:]))
    got_tiles = [send_tile(t, k) for k, t in enumerate(ivar[:-1])]
    weight_map = lax.optimization_barrier(functools.reduce(jnp.add, got_tiles, ivar[-1]))
    image, near, far = pl.pallas_call(
        image_body,
        out_shape=[arr(BC, rows_dev, side)] + [arr(BC, HALO, side)] * 2,
        in_specs=[SMEM] * 2 + [VMEM] * (1 + visits),
        out_specs=[VMEM] * 3,
        scratch_shapes=[pltpu.VMEM((BR * BC + 1, side, side), F32)],
        compiler_params=params,
        name="image",
    )(ids, slots, got_flux, *ivar)
    pairs = [(i + 1, i + 2) for i in range(0, owners - 2, 2)]
    far = lax.ppermute(far, "bulk", pairs + [(j, i) for i, j in pairs])
    near = lax.ppermute(near, "bulk", [(i, i ^ 1) for i in range(owners)])

    def convolve(first, count):
        return pl.pallas_call(
            functools.partial(conv_body, first, visits),
            out_shape=[tile] * count,
            in_specs=[SMEM] + [VMEM] * (8 + count),
            out_specs=[VMEM] * count,
            scratch_shapes=[pltpu.VMEM((2 * freqs, (per_tile + 1) * side), F32)],
            compiler_params=params,
        )(ids, near, image, far, spec, row_fwd, col_fwd, col_inv, row_inv, *ivar[first : first + count])

    last = visits - 1
    parts = convolve(0, 1)
    got = [send_tile(parts[0], 0)]
    parts = convolve(1, visits - 2)
    got += [send_tile(part, k + 1) for k, part in enumerate(parts)]
    numerator = functools.reduce(jnp.add, got, convolve(last, 1)[0])
    return (numerator / jnp.maximum(weight_map, 1.0), weight_map)


def solution(mesh):
    placed = (
        P("visit", "bulk", None, None, None),
        P("visit", "bulk", None, None, None),
        P("visit", "bulk", None, None, None),
        P("visit", "bulk", None, None, None),
        P("visit", "bulk", None, None),
        P("visit", "bulk", None),
        P("visit", "bulk", None, None),
        P(),
        P("visit", None),
    )
    return jax.shard_map(
        coadd_patches,
        mesh=mesh,
        in_specs=placed,
        out_specs=(P("bulk", "visit"), P("bulk", "visit")),
        check_vma=False,
    )
```

```python
import functools
import math

import jax
import jax.numpy as jnp
import numpy as np
from jax import lax
from jax.experimental import pallas as pl
from jax.experimental.pallas import tpu as pltpu
from jax.sharding import PartitionSpec as P


HALO = 64
BR = 2
BC = 8
CAP = 2
LANES = 128
VMEM_BYTES = 8 * 2**20
META = 8


F32 = jnp.float32
BF16 = jnp.bfloat16
VMEM = pl.BlockSpec(memory_space=pltpu.VMEM)
SMEM = pl.BlockSpec(memory_space=pltpu.SMEM)


def split(value):
    high = value.astype(BF16)
    low = (value - high.astype(F32)).astype(BF16)
    return high, low


def data(value, axis):
    high, low = split(value)
    return jnp.concatenate([high, low, high], axis)


def weights(value, axis):
    high, low = split(value)
    return jnp.concatenate([high, high, low], axis)


def table(value):
    value = np.asarray(value, np.float32)
    high = value.astype(jnp.bfloat16)
    return np.stack([high, (value - high.astype(np.float32)).astype(jnp.bfloat16)])


def fixed(ref, axis):
    return jnp.concatenate([ref[0], ref[0], ref[1]], axis)


def dot(a, b, dims=((1,), (0,))):
    return lax.dot_general(a, b, (dims, ((), ())), preferred_element_type=F32)


@functools.lru_cache
def make_tables(rows_dev, taps):
    length = rows_dev + taps - 1
    freqs = (length + 1) // 2
    k = np.arange(freqs)[:, None]

    def wave(first, second, period):
        return 2.0 * math.pi * ((first * second) % period) / period

    n = np.arange(rows_dev + 2 * HALO)[None, :] - 1
    theta = wave(k, n, length)
    used = n >= 0
    row_fwd = np.concatenate([np.cos(theta) * used, -np.sin(theta) * used], 0)
    theta = wave(k, np.arange(taps)[None, :], length)
    row_ker = np.concatenate([np.cos(theta), -np.sin(theta)], 0)
    period = 2 * taps
    n = np.arange(taps)[:, None]
    f = np.arange(taps)[None, :]
    col_fwd = []
    col_inv = []
    for odd in (0, 1):
        theta = wave(n, 2 * f + odd, period)
        c, s = np.cos(theta), np.sin(theta)
        col_fwd.append(np.block([[c, -s], [s, c]]))
        c, s = c.T, s.T
        sign = -1.0 if odd else 1.0
        col_inv.append(sign * np.block([[c, s], [-s, c]]))
    p = np.arange(rows_dev)[:, None] + taps - 1
    theta = wave(p, k.T, length)
    weight = np.where(k.T == 0, 1.0, 2.0) / (length * period)
    row_inv = np.concatenate([weight * np.cos(theta), -weight * np.sin(theta)], 1)
    return (
        table(row_fwd),
        table(row_ker),
        np.stack([table(t) for t in col_fwd]),
        np.stack([table(t) for t in col_inv]),
        table(row_inv),
    )


def partner(me, other):
    return jnp.bitwise_xor(me, other)


def places(ids, owner, slot):
    for q in range(slot.shape[2]):
        own = owner[0, 0, 0, q]
        rank = jnp.int32(0)
        for earlier in range(q):
            rank = rank + (owner[0, 0, 0, earlier] == own).astype(jnp.int32)
        yield q, partner(ids[0], own), own, rank, slot[0, 0, q]


def tile_at(ids, k, tiles):
    return jnp.bitwise_xor(ids[1], tiles - 1 - k)


def masked(extent, ivar, q):
    row_at = lax.broadcasted_iota(jnp.int32, ivar.shape, 0)
    col_at = lax.broadcasted_iota(jnp.int32, ivar.shape, 1)
    valid = (row_at < extent[0, 0, 0, q]) & (col_at < extent[0, 0, 1, q])
    return jnp.where(valid, ivar, 0.0)


def run(copies):
    for copy in copies:
        copy.start()
    for copy in copies:
        copy.wait()


def warp_body(ids, owner, slot, extent, ivar_far, rows_far, cols_far, flux_far, *rest):
    *outs, flux_out, ivar, rows, cols, flux, send, sems = rest
    side = ivar.shape[3]
    far = (ivar_far, rows_far, cols_far, flux_far)
    near = (ivar, rows, cols, flux)
    copies = [pltpu.make_async_copy(a, b, sems.at[n]) for n, (a, b) in enumerate(zip(far, near))]
    for copy in copies:
        copy.start()
    for d in range(len(outs)):
        for rank in range(CAP):
            send[d, rank, side:, :] = jnp.full((META, side), -1.0, F32)
    for copy in copies:
        copy.wait()
    for q, to, own, rank, at in places(ids, owner, slot):
        weighted = masked(extent, ivar[0, 0, q], q)
        planes = jnp.concatenate([weighted * flux[0, 0, q], weighted], 0)
        mid = dot(data(planes, 1), weights(cols[0, 0, q], 1), ((1,), (1,)))
        mid = jnp.concatenate([mid[:side], mid[side:]], 1)
        done = dot(weights(rows[0, 0, q], 1), data(mid, 0))
        flux_out[own * CAP + rank] = done[:, :side]
        send[to, rank, :side, :] = done[:, side:]
        send[to, rank, side:, :] = jnp.full((META, side), at.astype(F32), F32)
    for d, out in enumerate(outs):
        out[...] = send[d]


def weight_body(ids, own, *rest):
    *rest, slot_out, acc, buf, sems = rest
    count = slot_out.shape[0] // CAP
    far, out = rest[: count - 1], rest[count - 1 :]
    run([pltpu.make_async_copy(ref, buf.at[d], sems.at[d]) for d, ref in enumerate(far)])
    got = [own] + [buf.at[d] for d in range(count - 1)]
    side = acc.shape[1]
    spare = acc.shape[0] - 1
    per_tile = out[0].shape[1] // side
    acc[...] = jnp.zeros(acc.shape, F32)
    slots = []
    for d in range(count):
        for rank in range(CAP):
            at = jnp.max(got[d][rank, side:, :]).astype(jnp.int32)
            slots.append(jnp.where(at < 0, spare, at))
    for n, at in enumerate(slots):
        d, rank = divmod(n, CAP)
        slot_out[partner(ids[0], d) * CAP + rank] = at
        acc[at] += got[d][rank, :side, :]
    for k in range(len(out)):
        for c in range(per_tile):
            for r in range(BR):
                block = acc[r * BC + tile_at(ids, k, len(out)) * per_tile + c]
                out[k][r * side : (r + 1) * side, c * side : (c + 1) * side] = block


def image_body(ids, slot, got, *rest):
    *tiles, image, near, far, acc = rest
    odd_strip = ids[0] % 2 == 1
    side = acc.shape[1]
    per_tile = tiles[0].shape[1] // side
    acc[...] = jnp.zeros(acc.shape, F32)
    for n in range(slot.shape[0]):
        acc[slot[n]] += got[n]
    for k, tile in enumerate(tiles):
        for c in range(per_tile):
            to = tile_at(ids, k, len(tiles)) * per_tile + c
            for r in range(BR):
                rows = slice(r * side, (r + 1) * side)
                weight = tile[rows, c * side : (c + 1) * side]
                image[to, rows, :] = acc[r * BC + to] / jnp.maximum(weight, 1.0)
            top, bottom = image[to, :HALO, :], image[to, -HALO:, :]
            near[to] = jnp.where(odd_strip, top, bottom)
            far[to] = jnp.where(odd_strip, bottom, top)


def beside(stacked):
    n = stacked.shape[0] // 2
    return jnp.concatenate([stacked[:n], stacked[n:]], 1)


def spectrum_body(coeffs, basis, row_ker, col_fwd, out):
    kernel = coeffs[0, 0] * basis[0]
    for k in range(1, basis.shape[0]):
        kernel = kernel + coeffs[0, k] * basis[k]
    lines = data(beside(dot(fixed(row_ker, 1), data(kernel, 0))), 1)
    for odd in (0, 1):
        out[odd] = dot(lines, fixed(col_fwd.at[odd], 0))


def conv_body(first, tiles, ids, near, image, far, spec, row_fwd, col_fwd, col_inv, row_inv, *rest):
    *rest, lines = rest
    count = len(rest) // 2
    weight, out = rest[:count], rest[count:]
    taps = image.shape[2]
    per_tile = out[0].shape[1] // taps
    freqs = spec.shape[1]
    odd_strip = ids[0] % 2 == 1

    def column(c):
        above = jnp.where(odd_strip, near[c], far[c])
        below = jnp.where(odd_strip, far[c], near[c])
        return jnp.concatenate([above, image[c], below], 0)

    lead = fixed(row_fwd, 1)
    last = fixed(row_inv, 1)
    for k in range(count):
        start = tile_at(ids, first + k, tiles) * per_tile
        parts = [column(start + c) for c in range(per_tile)]
        before = jnp.where(start > 0, column(jnp.maximum(start - 1, 0)), 0.0)
        after = jnp.where(start + per_tile < BC, column(jnp.minimum(start + per_tile, BC - 1)), 0.0)
        ext = jnp.concatenate([before[:, taps - HALO :], *parts, after[:, :HALO]], 1)
        lines[...] = dot(lead, data(ext, 0))
        one = [lines[:, c * taps : (c + 1) * taps] for c in range(per_tile + 1)]
        total = []
        for odd in (0, 1):
            mixed = [beside(a - b if odd else a + b) for a, b in zip(one, one[1:])]
            freq = dot(data(jnp.concatenate(mixed, 0), 1), fixed(col_fwd.at[odd], 0))
            kr = jnp.concatenate([spec[odd, :, :taps]] * per_tile, 0)
            ki = jnp.concatenate([spec[odd, :, taps:]] * per_tile, 0)
            zr, zi = freq[:, :taps], freq[:, taps:]
            prod = jnp.concatenate([zr * kr - zi * ki, zr * ki + zi * kr], 1)
            total.append(dot(data(prod, 1), fixed(col_inv.at[odd], 0)))
        wave = total[0] + total[1]
        parts = [wave[c * freqs : (c + 1) * freqs] for c in range(per_tile)]
        cols = [jnp.concatenate([p[:, :taps], p[:, taps:]], 0) for p in parts]
        out[k][...] = dot(last, data(jnp.concatenate(cols, 1), 0)) * weight[k][...]


def send_tile(tile, k):
    visits = lax.axis_size("visit")
    return lax.ppermute(tile, "visit", [(v, v ^ (visits - 1 - k)) for v in range(visits)])


def send_part(tile, route):
    return lax.ppermute(tile, "visit", route)


def coadd_patches(piece_flux, piece_ivar, warp_rows, warp_cols, piece_owner, piece_slot, piece_extent, basis, coeffs):
    owners = lax.axis_size("bulk")
    visits = lax.axis_size("visit")
    _, side = piece_flux.shape[2:4]
    assert side == LANES and side == 2 * HALO and owners & (owners - 1) == 0
    rows_dev = BR * side
    per_tile = BC // visits
    cap = owners * CAP
    row_fwd, row_ker, col_fwd, col_inv, row_inv = [jnp.asarray(t) for t in make_tables(rows_dev, side)]
    freqs = row_fwd.shape[1] // 2
    ids = jnp.stack([lax.axis_index("bulk"), lax.axis_index("visit")]).astype(jnp.int32)
    facts = (ids, piece_owner.transpose(0, 1, 3, 2), piece_slot, piece_extent.transpose(0, 1, 3, 2))

    params = pltpu.CompilerParams(vmem_limit_bytes=VMEM_BYTES + 12 * 4 * piece_flux.size)

    def arr(*shape):
        return jax.ShapeDtypeStruct(shape, F32)

    hbm = pl.BlockSpec(memory_space=pltpu.HBM)

    def in_hbm(*arrays):
        return [pltpu.with_memory_space_constraint(a, pltpu.HBM) for a in arrays]

    def exchange(sent):
        got = [sent[0]]
        for d in range(1, owners):
            got.append(lax.ppermute(sent[d], "bulk", [(i, i ^ d) for i in range(owners)]))
        return got

    *sent_weight, sent_flux = pl.pallas_call(
        warp_body,
        out_shape=[arr(CAP, side + META, side)] * owners + [arr(cap, side, side)],
        in_specs=[SMEM] * 4 + [hbm] * 4,
        out_specs=[VMEM] * (owners + 1),
        scratch_shapes=[pltpu.VMEM(piece_flux.shape, F32)] * 4
        + [pltpu.VMEM((owners, CAP, side + META, side), F32), pltpu.SemaphoreType.DMA((4,))],
        compiler_params=params,
        name="warp",
    )(*facts, *in_hbm(piece_ivar, warp_rows, warp_cols, piece_flux))
    got_weight = exchange(sent_weight)
    got_flux = lax.all_to_all(sent_flux, "bulk", split_axis=0, concat_axis=0, tiled=True)
    spec = pl.pallas_call(
        spectrum_body,
        out_shape=arr(2, freqs, 2 * side),
        in_specs=[SMEM] + [VMEM] * 3,
        out_specs=VMEM,
        compiler_params=params,
        name="spectrum",
    )(coeffs, basis, row_ker, col_fwd)
    tile = arr(rows_dev, per_tile * side)
    *ivar, slots = pl.pallas_call(
        weight_body,
        out_shape=[tile] * visits + [jax.ShapeDtypeStruct((cap,), jnp.int32)],
        in_specs=[SMEM, VMEM] + [hbm] * (owners - 1),
        out_specs=[VMEM] * visits + [SMEM],
        scratch_shapes=[
            pltpu.VMEM((BR * BC + 1, side, side), F32),
            pltpu.VMEM((owners - 1, CAP, side + META, side), F32),
            pltpu.SemaphoreType.DMA((owners - 1,)),
        ],
        compiler_params=params,
        name="weights",
    )(ids, got_weight[0], *in_hbm(*got_weight[1:]))
    got_tiles = [send_tile(t, k) for k, t in enumerate(ivar[:-1])]
    weight_map = lax.optimization_barrier(functools.reduce(jnp.add, got_tiles, ivar[-1]))
    image, near, far = pl.pallas_call(
        image_body,
        out_shape=[arr(BC, rows_dev, side)] + [arr(BC, HALO, side)] * 2,
        in_specs=[SMEM] * 2 + [VMEM] * (1 + visits),
        out_specs=[VMEM] * 3,
        scratch_shapes=[pltpu.VMEM((BR * BC + 1, side, side), F32)],
        compiler_params=params,
        name="image",
    )(ids, slots, got_flux, *ivar)
    pairs = [(i + 1, i + 2) for i in range(0, owners - 2, 2)]
    far = lax.ppermute(far, "bulk", pairs + [(j, i) for i, j in pairs])
    near = lax.ppermute(near, "bulk", [(i, i ^ 1) for i in range(owners)])

    def convolve(first, count):
        return pl.pallas_call(
            functools.partial(conv_body, first, visits),
            out_shape=[tile] * count,
            in_specs=[SMEM] + [VMEM] * (8 + count),
            out_specs=[VMEM] * count,
            scratch_shapes=[pltpu.VMEM((2 * freqs, (per_tile + 1) * side), F32)],
            compiler_params=params,
        )(ids, near, image, far, spec, row_fwd, col_fwd, col_inv, row_inv, *ivar[first : first + count])

    first, *_ = convolve(0, 1)
    if visits == 4:
        joining = send_part(first, [(0, 1), (3, 2)])
        got = [send_part(first, [(1, 2), (2, 1)])]
        second, third = convolve(1, 2)
        got.append(send_part(third, [(0, 1), (1, 0), (2, 3), (3, 2)]))
        got.append(send_part(second + joining, [(0, 2), (1, 3), (2, 0), (3, 1)]))
    else:
        got = [send_tile(first, 0)]
        middle = convolve(1, visits - 2)
        got += [send_tile(part, k + 1) for k, part in enumerate(middle)]
    numerator = functools.reduce(jnp.add, got, convolve(visits - 1, 1)[0])
    return (numerator / jnp.maximum(weight_map, 1.0), weight_map)


def solution(mesh):
    placed = (
        P("visit", "bulk", None, None, None),
        P("visit", "bulk", None, None, None),
        P("visit", "bulk", None, None, None),
        P("visit", "bulk", None, None, None),
        P("visit", "bulk", None, None),
        P("visit", "bulk", None),
        P("visit", "bulk", None, None),
        P(),
        P("visit", None),
    )
    return jax.shard_map(
        coadd_patches,
        mesh=mesh,
        in_specs=placed,
        out_specs=(P("bulk", "visit"), P("bulk", "visit")),
        check_vma=False,
    )
```
